32 devices in a mesh: row: 4 (over y, x), col: 8 (over z, core).
Axes of the slice: x: 2, y: 2, z: 4, core: 2. Of those that a mesh axis runs over, the one named last changes fastest.
Arguments:
- features: bfloat16 [8192, 512], P(('row', 'col')), may hold values from -40 to 40
- w_query: bfloat16 [512, 512], replicated, may hold values from -0.25 to 0.25
- w_key: bfloat16 [512, 512], replicated, may hold values from -0.25 to 0.25
- w_value: bfloat16 [512, 512], replicated, may hold values from -0.25 to 0.25
- w_out: bfloat16 [512, 512], replicated, may hold values from -0.25 to 0.25
- pairs: int32 [4, 8, 128, 2], P('row', 'col'), may hold values from 0 to 15, as said below
- counts: int32 [4, 8], P('row', 'col'), may hold values from 16 to 128, as said below
- masks: int32 [4, 8, 128, 128, 4], P('row', 'col'), may hold values from -2147483648 to 2147483646, as said below
Outputs:
- updated: bfloat16 [8192, 512], P(('row', 'col'))
The draws below stay inside these ranges and needn't reach their ends.
Inputs may be any that keep to these rules, and one draw needn't show every extreme that they name: Within one device's list all 128 entries are distinct pairs; the first column is a query tile below 16, the second a key tile below 8. `counts`: some device has a full list of 128 entries in every draw. `masks`: any 32-bit pattern.
All inputs are finite; a program needn't handle non-finite values.
Results may differ from the reference program's by a relative error of at most 0.012.
The reference program's roundings to bfloat16 on the way count: a program that leaves them out, or rounds other values in their place, can miss the bound.
Values may be sent and summed in bfloat16 or wider, within the bound.
A program may use at most 128 MiB of HBM per device.

```python
import math
import jax
import jax.numpy as jnp
from jax import lax

D = 512
HEADS = 8
HEAD_DIM = 64
TILE = 128
MAXB = 128
NODE_DEV = 256
NODES = 8192
QTILES = 16
KTILES = 8
N_ROW = 4
N_COL = 8


def draw_features(key, part):
    base = jax.random.normal(key, (NODES, D), jnp.float32)
    return jnp.clip(base, -4.0, 4.0).astype(jnp.bfloat16)


def draw_pairs(key, part):
    keys = jax.random.split(jax.random.fold_in(key, 11), N_ROW * N_COL)
    ident = jax.vmap(lambda single: jax.random.permutation(single, QTILES * KTILES)[:MAXB])(keys)
    table = jnp.stack([ident // KTILES, ident % KTILES], -1).astype(jnp.int32)
    return table.reshape(N_ROW, N_COL, MAXB, 2)


def draw_counts(key, part):
    first = jax.random.randint(jax.random.fold_in(key, 1), (N_ROW * N_COL,), 0, MAXB)
    second = jax.random.randint(jax.random.fold_in(key, 2), (N_ROW * N_COL,), 0, MAXB)
    lowest = max(1, MAXB // 8)
    values = jnp.maximum(jnp.minimum(first, second) + 1, lowest)
    chosen = jax.random.randint(jax.random.fold_in(key, 3), (), 0, N_ROW * N_COL)
    values = jnp.where(jnp.arange(N_ROW * N_COL, dtype=jnp.int32) == chosen, MAXB, values)
    return values.astype(jnp.int32).reshape(N_ROW, N_COL)


def draw_masks(key, part):
    shape = (N_ROW, N_COL, MAXB, TILE, TILE // 32)
    return jax.random.randint(jax.random.fold_in(key, 5), shape, -2147483648, 2147483647, jnp.int32)


def noise(stream_key, extent, spread, bound, kind=jnp.bfloat16):
    return jnp.clip(spread * jax.random.normal(stream_key, extent, jnp.float32), -bound, bound).astype(kind)


def setup_inputs(seed: int = 0) -> dict:
    seeds = jax.random.split(jax.random.key(seed), 9)
    features = draw_features(jax.random.fold_in(seeds[8], 71), 0)
    w_query = noise(seeds[1], (D, D), D ** -0.5, 0.25)
    w_key = noise(seeds[2], (D, D), D ** -0.5, 0.25)
    w_value = noise(seeds[3], (D, D), D ** -0.5, 0.25)
    w_out = noise(seeds[4], (D, D), D ** -0.5, 0.25)
    pairs = draw_pairs(jax.random.fold_in(seeds[8], 71), 0)
    counts = draw_counts(jax.random.fold_in(seeds[8], 71), 0)
    masks = draw_masks(jax.random.fold_in(seeds[8], 71), 0)
    return dict(features=features, w_query=w_query, w_key=w_key, w_value=w_value, w_out=w_out, pairs=pairs, counts=counts, masks=masks)


def unpack_bits(words):
    shifts = jnp.broadcast_to(jnp.arange(32, dtype=jnp.int32), words.shape + (32,))
    bits = lax.shift_right_logical(words[..., None], shifts) & 1
    return bits.reshape(words.shape[:-1] + (words.shape[-1] * 32,)) == 1

def device_partial(q_part, k_part, v_part, my_pairs, my_count, my_words):
    scale = 1.0 / math.sqrt(HEAD_DIM)
    tiles_q = q_part.reshape(QTILES, TILE, HEADS, HEAD_DIM)
    tiles_k = k_part.reshape(KTILES, TILE, HEADS, HEAD_DIM)
    tiles_v = v_part.reshape(KTILES, TILE, HEADS, HEAD_DIM)
    qsel = my_pairs[:, 0]
    ksel = my_pairs[:, 1]
    q_blk = tiles_q[qsel].astype(jnp.float32)
    k_blk = tiles_k[ksel].astype(jnp.float32)
    v_blk = tiles_v[ksel].astype(jnp.float32)
    scores = jnp.einsum('gihd,gjhd->ghij', q_blk, k_blk) * scale
    valid = jnp.arange(MAXB, dtype=jnp.int32) < my_count
    live = unpack_bits(my_words) & valid[:, None, None]
    masked = jnp.where(live[:, None], scores, -jnp.inf)
    rowmax = masked.max(-1)
    tmax = jnp.zeros((QTILES, HEADS, TILE), jnp.float32).at[qsel].max(rowmax)
    prob = jnp.where(live[:, None], jnp.exp(scores - tmax[qsel][..., None]), 0.0).astype(jnp.bfloat16)
    probf = prob.astype(jnp.float32)
    den = jnp.exp(-tmax).at[qsel].add(probf.sum(-1))
    weighted = jnp.einsum('ghij,gjhd->gihd', probf, v_blk)
    num = jnp.zeros((QTILES, TILE, HEADS, HEAD_DIM), jnp.float32).at[qsel].add(weighted)
    return (tmax, num, den)

def reference(features, w_query, w_key, w_value, w_out, pairs, counts, masks):
    queries = jnp.dot(features, w_query, preferred_element_type=jnp.float32).astype(jnp.bfloat16)
    keys = jnp.dot(features, w_key, preferred_element_type=jnp.float32).astype(jnp.bfloat16)
    values = jnp.dot(features, w_value, preferred_element_type=jnp.float32).astype(jnp.bfloat16)
    q_rows = NODE_DEV * N_COL
    k_rows = NODE_DEV * N_ROW
    keys_grid = keys.reshape(N_ROW, N_COL, NODE_DEV, D)
    values_grid = values.reshape(N_ROW, N_COL, NODE_DEV, D)

    def per_row(r):
        q_part = lax.dynamic_slice_in_dim(queries, (r * q_rows).astype(jnp.int32), q_rows, 0)

        def per_col(c):
            k_part = lax.dynamic_index_in_dim(keys_grid, c, 1, keepdims=False).reshape(k_rows, D)
            v_part = lax.dynamic_index_in_dim(values_grid, c, 1, keepdims=False).reshape(k_rows, D)
            tmax, num, den = device_partial(q_part, k_part, v_part, pairs[r, c], counts[r, c], masks[r, c])
            part = (num / den.transpose(0, 2, 1)[..., None]).astype(jnp.bfloat16).astype(jnp.float32)
            return (tmax, part, den)
        tmax, part, den = lax.map(per_col, jnp.arange(N_COL, dtype=jnp.int32))
        top = tmax.max(0)
        weight = jnp.exp(tmax - top) * den
        total = weight.sum(0)
        numer = (part * weight.transpose(0, 1, 3, 2)[..., None]).sum(0)
        attended = (numer / total.transpose(0, 2, 1)[..., None]).astype(jnp.bfloat16).reshape(q_rows, D)
        return jnp.dot(attended, w_out, preferred_element_type=jnp.float32).astype(jnp.bfloat16)
    result = lax.map(per_row, jnp.arange(N_ROW, dtype=jnp.int32))
    return result.reshape(NODES, D)
```

```python
import functools
import math

import jax
import jax.numpy as jnp
from jax import lax
from jax.experimental import pallas as pl
from jax.experimental.pallas import tpu as pltpu
from jax.sharding import PartitionSpec as P

HEADS = 8
TILE = 128
BLOCK = 512
ONES = 16
PIECES = 2


def build_bias(words_ref, first, bias_ref):
    keys, span = bias_ref.shape
    k_tiles = keys // TILE
    tiles = span // TILE
    shift = 31 - lax.broadcasted_iota(jnp.int32, (32, TILE), 0)
    for b in range(k_tiles):
        for t in range(tiles):
            words = words_ref[(first + t) * k_tiles + b]
            for j in range(TILE // 32):
                bits = jnp.broadcast_to(words[j : j + 1, :], (32, TILE)) << shift
                bias_ref[pl.ds(b * TILE + j * 32, 32), pl.ds(t * TILE, TILE)] = jnp.where(
                    bits < 0, 0.0, -jnp.inf
                )


def attend_group(queries, k_ref, v_ref, part_ref, stat_ref, bias_ref, score_ref):
    width, span = queries.shape
    keys = k_ref.shape[0]
    head = width // HEADS
    scale = 1.0 / math.sqrt(head)
    factor = scale * math.log2(math.e)
    v_rows = v_ref.shape[0] // HEADS
    step = min(BLOCK, keys)
    blocks = keys // step
    upper = lax.broadcasted_iota(jnp.int32, (2 * head, span), 0) < head

    def scores(h, block, top):
        pair = h // 2
        both = queries[pair * 2 * head : (pair + 1) * 2 * head, :]
        mine = jnp.where(upper == (h % 2 == 0), both, jnp.zeros_like(both))
        rows = slice(block * step, (block + 1) * step)
        raw = jnp.dot(
            k_ref[rows, pair * 2 * head : (pair + 1) * 2 * head],
            mine,
            preferred_element_type=jnp.float32,
        )
        raw = raw + bias_ref[rows, :]
        score_ref[h % 2, rows, :] = raw
        return jnp.maximum(top, jnp.max(raw.reshape(step // 8, 8, span), axis=0))

    def weighted(h, block, top, total):
        rows = slice(block * step, (block + 1) * step)
        prob = jnp.exp2((score_ref[h % 2, rows, :] - top) * factor).astype(jnp.bfloat16)
        term = jnp.dot(
            v_ref[h * v_rows : (h + 1) * v_rows, rows], prob, preferred_element_type=jnp.float32
        )
        return term if total is None else total + term

    def finish(h, top, total):
        peak = top * scale
        den = total[head : head + 1, :] + jnp.exp(-peak)
        part_ref[h * head : (h + 1) * head, :] = (total[:head, :] / den).astype(jnp.bfloat16)
        stat_ref[h : h + 1, :] = peak
        stat_ref[HEADS + h : HEADS + h + 1, :] = den

    zero = jnp.zeros((8, span), jnp.float32)
    tops = zero
    for block in range(blocks):
        tops = scores(0, block, tops)
    for h in range(HEADS):
        top = jnp.max(tops, axis=0, keepdims=True)
        total, tops = None, zero
        for block in range(blocks):
            if h + 1 < HEADS:
                tops = scores(h + 1, block, tops)
            total = weighted(h, block, top, total)
        finish(h, top, total)


MESH = pl.DeviceIdType.MESH
GROUPS = 4


def fused_kernel(
    rows,
    cols,
    table_ref,
    masks_ref,
    features_ref,
    wq_ref,
    wk_ref,
    wv_ref,
    out_ref,
    kf,
    qf,
    wq_t,
    wv_t,
    words_out,
    words,
    k_all,
    v_all,
    q_all,
    part,
    stat,
    mate_part,
    mate_stat,
    both_part,
    both_stat,
    fin_part,
    fin_stat,
    bias,
    score,
    q_send,
    q_recv,
    z_send,
    z_recv,
    row_send,
    row_recv,
    word_send,
    word_recv,
    pair_send,
    pair_recv,
    fin_send,
    fin_recv,
):
    nodes, width = features_ref.shape
    head = width // HEADS
    f32 = jnp.float32
    chips = cols // 2
    planes = chips // 2
    last = planes - 1
    turns = planes * GROUPS
    size = nodes // PIECES
    r, c = lax.axis_index("row"), lax.axis_index("col")
    m, k = c // 2, lax.rem(c, 2)
    other = m + 1 - 2 * lax.rem(m, 2)
    mate = (r, m * 2 + 1 - k)
    partner = (r, other * 2 + k)

    def reader(j):
        return lax.rem(m + chips - 2 * j, chips)

    def flip(place, b):
        return place + 1 - 2 * lax.rem(place, 2) if b else place

    def row_to(d):
        if rows % 2:
            return lax.rem(r + d, rows)
        return flip(lax.rem(r + d // 2 * 2, rows), d % 2)

    def row_from(d):
        if rows % 2:
            return lax.rem(r + rows - d, rows)
        return lax.rem(flip(r, d % 2) + rows - d // 2 * 2, rows)

    def send(src, dst, send_sem, recv_sem, device):
        return pltpu.make_async_remote_copy(
            src_ref=src,
            dst_ref=dst,
            send_sem=send_sem,
            recv_sem=recv_sem,
            device_id=device,
            device_id_type=MESH,
        )

    barrier = pltpu.get_barrier_semaphore()
    peers = [mate, partner]
    peers += [(lax.rem(r + d, rows), c) for d in range(1, rows)]
    peers += [(r, reader(j) * 2 + k) for j in range(1, planes)]
    for peer in peers:
        pl.semaphore_signal(barrier, inc=1, device_id=peer, device_id_type=MESH)
    pl.semaphore_wait(barrier, len(peers))

    def query_copy(step):
        if step == 0:
            return send(features_ref, qf.at[1], q_send.at[0], q_recv.at[1], mate)
        if step == 1:
            return send(features_ref, qf.at[2], q_send.at[1], q_recv.at[2], partner)
        return send(qf.at[2], qf.at[3], q_send.at[2], q_recv.at[3], mate)

    def line_copy(j, piece):
        span = pl.ds(piece * size, size)
        return send(
            features_ref.at[span],
            kf.at[j, r, span],
            z_send.at[j, piece],
            z_recv.at[j, piece],
            (r, reader(j) * 2 + k),
        )

    def row_copy(j, d, piece, own=False):
        span = pl.ds(piece * size, size)
        return send(
            features_ref.at[span] if own else kf.at[j, r, span],
            kf.at[j, r, span],
            row_send.at[j, d, piece],
            row_recv.at[j, r, piece],
            (row_to(d), c),
        )

    def word_copy(j):
        return send(
            words_out.at[j - 1],
            words.at[j],
            word_send.at[j],
            word_recv.at[j],
            (r, reader(j) * 2 + k),
        )

    query_copy(1).start()
    for j in range(1, planes):
        for piece in range(PIECES):
            line_copy(j, piece).start()
    for piece in range(PIECES):
        for d in range(1, rows):
            row_copy(0, d, piece, True).start()
    query_copy(0).start()

    k_tiles = rows * nodes // TILE
    entries = 2 * 2 * (nodes // TILE) * k_tiles

    def gather_words(j, dst):
        first = reader(j) // 2 * entries

        def step(s, carry):
            for u in range(8):
                e = s * 8 + u
                entry = table_ref[first + e]
                dst[e] = masks_ref[jnp.maximum(entry, 0)] * jnp.where(entry >= 0, 1, 0)
            return carry

        lax.fori_loop(0, entries // 8, step, 0)

    for j in range(1, planes):
        gather_words(j, words_out.at[j - 1])
        word_copy(j).start()

    kf[0, r] = features_ref[...]
    qf[0] = features_ref[...]
    wq_t[...] = wq_ref[...].T
    wv_t[...] = wv_ref[...].T
    for j in range(planes):
        for h in range(HEADS):
            v_all[j, h * (head + ONES) + head : (h + 1) * (head + ONES), :] = jnp.ones(
                (ONES, rows * nodes), jnp.bfloat16
            )
    gather_words(0, words.at[0])

    def project_row(j, slot):
        block = kf[j, slot]
        lane = pl.ds(pl.multiple_of(slot * nodes, nodes), nodes)
        k_all[j, lane, :] = jnp.dot(block, wk_ref[...], preferred_element_type=f32).astype(
            jnp.bfloat16
        )
        value = lax.dot_general(
            wv_t[...], block, (((1,), (1,)), ((), ())), preferred_element_type=f32
        ).astype(jnp.bfloat16)
        for h in range(HEADS):
            v_all[j, h * (head + ONES) : h * (head + ONES) + head, lane] = value[
                h * head : (h + 1) * head, :
            ]

    def await_row(j, slot):
        for piece in range(PIECES):
            span = pl.ds(piece * size, size)
            send(
                kf.at[j, slot, span],
                kf.at[j, slot, span],
                row_send.at[0, 0, 0],
                row_recv.at[j, slot, piece],
                mate,
            ).wait_recv()

    project_row(0, r)
    for d in range(1, rows):
        await_row(0, row_from(d))
        project_row(0, row_from(d))

    def relay(j, piece):
        line_copy(j, piece).wait_recv()
        for d in range(1, rows):
            row_copy(j, d, piece).start()

    def pair_copies(i, j, which):
        return (
            send(
                part.at[i],
                mate_part.at[j, which],
                pair_send.at[j, which, 0],
                pair_recv.at[j, which, 0],
                mate,
            ),
            send(
                stat.at[i],
                mate_stat.at[j, which],
                pair_send.at[j, which, 1],
                pair_recv.at[j, which, 1],
                mate,
            ),
        )

    fin_copies = (
        send(both_part, fin_part, fin_send.at[0], fin_recv.at[0], partner),
        send(both_stat, fin_stat, fin_send.at[1], fin_recv.at[1], partner),
    )

    def weigh(sources):
        peaks = [ref[0:HEADS, :] for _, ref in sources]
        top = functools.reduce(jnp.maximum, peaks)
        weights = [
            jnp.exp(peak - top) * ref[HEADS : 2 * HEADS, :]
            for peak, (_, ref) in zip(peaks, sources)
        ]
        total = functools.reduce(jnp.add, weights)
        return top, weights, total

    def blend(sources, weights, total, h):
        rows_of = slice(h * head, (h + 1) * head)
        numer = functools.reduce(
            jnp.add,
            [
                ref[rows_of, :].astype(f32) * weight[h : h + 1, :]
                for weight, (ref, _) in zip(weights, sources)
            ],
        )
        return (numer / total[h : h + 1, :]).astype(jnp.bfloat16)

    def gathered(which):
        sources = []
        for j in range(planes):
            for copy in pair_copies(0, j, which):
                copy.wait_recv()
            i = j * GROUPS + (2 * which if j < last else GROUPS - 1 - 2 * which)
            sources.append((part.at[i], stat.at[i]))
            sources.append((mate_part.at[j, which], mate_stat.at[j, which]))
        return sources

    def turn(i, carry):
        j = i // GROUPS
        t = lax.rem(i, GROUPS)
        slot = jnp.where(j == last, GROUPS - 1 - t, t)
        chip = jnp.where(slot < 2, m, other)
        lane = jnp.where(lax.rem(slot, 2) == 0, k, 1 - k)
        tile = (lax.rem(chip, 2) * 2 + lane) * (nodes // TILE)

        @pl.when(i == min(1, last))
        def _():
            query_copy(1).wait_recv()
            query_copy(2).start()

        for piece in range(PIECES):
            for plane in range(1, planes):

                @pl.when(i == (plane - 1) * GROUPS + piece)
                def _():
                    relay(plane, piece)

        @pl.when((t == 0) & (j > 0))
        def _():
            project_row(j, r)
            for d in range(1, rows):
                await_row(j, row_from(d))
                project_row(j, row_from(d))
            send(
                words.at[j], words.at[j], word_send.at[j], word_recv.at[j], mate
            ).wait_recv()

        @pl.when((j == 0) & (lax.rem(slot, 2) == 1))
        def _():
            send(qf.at[slot], qf.at[slot], q_send.at[0], q_recv.at[slot], mate).wait_recv()

        @pl.when(j == 0)
        def _():
            q_all[slot] = lax.dot_general(
                wq_t[...], qf[slot], (((1,), (1,)), ((), ())), preferred_element_type=f32
            ).astype(jnp.bfloat16)

        build_bias(words.at[j], tile, bias)

        @pl.when(i == last * GROUPS + 2)
        def _():
            sources = gathered(1)
            top, weights, total = weigh(sources)
            both_stat[0:HEADS, :] = top
            both_stat[HEADS : 2 * HEADS, :] = total
            for h in range(HEADS):
                both_part[h * head : (h + 1) * head, :] = blend(sources, weights, total, h)
            for copy in fin_copies:
                copy.start()

        attend_group(
            q_all.at[slot], k_all.at[j], v_all.at[j], part.at[i], stat.at[i], bias, score
        )

        @pl.when(lax.rem(slot, 2) == 1)
        def _():
            for copy in pair_copies(i, j, slot // 2):
                copy.start()

        return carry

    lax.fori_loop(0, turns, turn, 0)

    sources = gathered(0)
    for copy in fin_copies:
        copy.wait_recv()
    sources.append((fin_part, fin_stat))
    _, weights, total = weigh(sources)
    for h in range(HEADS):
        out_ref[h * head : (h + 1) * head, :] = blend(sources, weights, total, h)

    for step in range(3):
        query_copy(step).wait_send()
    for piece in range(PIECES):
        for d in range(1, rows):
            row_copy(0, d, piece, True).wait_send()
            for j in range(1, planes):
                row_copy(j, d, piece).wait_send()
        for j in range(1, planes):
            line_copy(j, piece).wait_send()
    for j in range(1, planes):
        word_copy(j).wait_send()
    for j in range(planes):
        for which in range(2):
            for copy in pair_copies(0, j, which):
                copy.wait_send()
    for copy in fin_copies:
        copy.wait_send()


def fused(mesh_shape, table, masks, features, w_query, w_key, w_value):
    rows, cols = mesh_shape["row"], mesh_shape["col"]
    planes = cols // 4
    turns = planes * GROUPS
    nodes, width = features.shape
    keys = rows * nodes
    head = width // HEADS
    entries = 2 * 2 * (nodes // TILE) * (keys // TILE)
    bf16, f32, i32 = jnp.bfloat16, jnp.float32, jnp.int32
    whole = pl.BlockSpec(memory_space=pltpu.VMEM)
    dma = pltpu.SemaphoreType.DMA
    return pl.pallas_call(
        functools.partial(fused_kernel, rows, cols),
        out_shape=jax.ShapeDtypeStruct((width, nodes), bf16),
        in_specs=[pl.BlockSpec(memory_space=pltpu.SMEM)] + [whole] * 5,
        out_specs=whole,
        scratch_shapes=[
            pltpu.VMEM((planes, rows, nodes, width), bf16),
            pltpu.VMEM((GROUPS, nodes, width), bf16),
            pltpu.VMEM((width, width), bf16),
            pltpu.VMEM((width, width), bf16),
            pltpu.VMEM((max(planes - 1, 1), entries, TILE // 32, TILE), i32),
            pltpu.VMEM((planes, entries, TILE // 32, TILE), i32),
            pltpu.VMEM((planes, keys, width), bf16),
            pltpu.VMEM((planes, HEADS * (head + ONES), keys), bf16),
            pltpu.VMEM((GROUPS, width, nodes), bf16),
            pltpu.VMEM((turns, width, nodes), bf16),
            pltpu.VMEM((turns, 2 * HEADS, nodes), f32),
            pltpu.VMEM((planes, 2, width, nodes), bf16),
            pltpu.VMEM((planes, 2, 2 * HEADS, nodes), f32),
            pltpu.VMEM((width, nodes), bf16),
            pltpu.VMEM((2 * HEADS, nodes), f32),
            pltpu.VMEM((width, nodes), bf16),
            pltpu.VMEM((2 * HEADS, nodes), f32),
            pltpu.VMEM((keys, nodes), f32),
            pltpu.VMEM((2, keys, nodes), f32),
            dma((3,)),
            dma((GROUPS,)),
            dma((planes, PIECES)),
            dma((planes, PIECES)),
            dma((planes, rows, PIECES)),
            dma((planes, rows, PIECES)),
            dma((planes,)),
            dma((planes,)),
            dma((planes, 2, 2)),
            dma((planes, 2, 2)),
            dma((2,)),
            dma((2,)),
        ],
        compiler_params=pltpu.CompilerParams(
            collective_id=0, has_side_effects=True, vmem_limit_bytes=60 * 1024 * 1024
        ),
        name="fused",
    )(table, masks, features, w_query, w_key, w_value)


def entry_table(pairs, count, q_tiles, k_tiles):
    entries = pairs.shape[0]
    ids = lax.broadcasted_iota(jnp.int32, (q_tiles * k_tiles, entries), 1)
    cell = lax.broadcasted_iota(jnp.int32, (q_tiles * k_tiles, entries), 0)
    code = (pairs[:, 0] * k_tiles + pairs[:, 1])[None, :]
    return jnp.max(jnp.where((code == cell) & (ids < count), ids, -1), axis=1)


def body(mesh_shape, features, w_query, w_key, w_value, w_out, pairs, counts, masks):
    nodes = features.shape[0]
    rows, cols = mesh_shape["row"], mesh_shape["col"]
    table = entry_table(pairs[0, 0], counts[0, 0], cols * nodes // TILE, rows * nodes // TILE)
    words = masks[0, 0].transpose(0, 2, 1)
    attended = fused(mesh_shape, table, words, features, w_query, w_key, w_value)
    return lax.dot_general(
        attended, w_out, (((0,), (0,)), ((), ())), preferred_element_type=jnp.float32
    ).astype(jnp.bfloat16)


def solution(mesh):
    in_specs = (
        P(("row", "col"), None),
        P(),
        P(),
        P(),
        P(),
        P("row", "col", None, None),
        P("row", "col"),
        P("row", "col", None, None, None),
    )
    out_specs = P(("row", "col"), None)
    return jax.shard_map(
        functools.partial(body, dict(mesh.shape)), mesh=mesh, in_specs=in_specs, out_specs=out_specs, check_vma=False)
```

```python
import functools
import math

import jax
import jax.numpy as jnp
from jax import lax
from jax.experimental import pallas as pl
from jax.experimental.pallas import tpu as pltpu
from jax.sharding import PartitionSpec as P

HEADS = 8
TILE = 128
BLOCK = 512
ONES = 16


def build_bias(words_ref, first, k_tiles, spots, bias_ref):
    span = bias_ref.shape[1]
    tiles = span // TILE
    shift = 31 - lax.broadcasted_iota(jnp.int32, (32, TILE), 0)
    for b, spot in enumerate(spots):
        for t in range(tiles):
            words = words_ref[first + t * k_tiles + spot]
            for j in range(TILE // 32):
                bits = jnp.broadcast_to(words[j : j + 1, :], (32, TILE)) << shift
                bias_ref[pl.ds(b * TILE + j * 32, 32), pl.ds(t * TILE, TILE)] = jnp.where(
                    bits < 0, 0.0, -jnp.inf
                )


def attend_group(queries, k_ref, v_ref, part_ref, stat_ref, bias_ref, score_ref):
    width, span = queries.shape
    keys = k_ref.shape[0]
    head = width // HEADS
    scale = 1.0 / math.sqrt(head)
    factor = scale * math.log2(math.e)
    v_rows = v_ref.shape[0] // HEADS
    step = min(BLOCK, keys)
    blocks = keys // step
    upper = lax.broadcasted_iota(jnp.int32, (2 * head, span), 0) < head

    def scores(h, block, top):
        pair = h // 2
        both = queries[pair * 2 * head : (pair + 1) * 2 * head, :]
        mine = jnp.where(upper == (h % 2 == 0), both, jnp.zeros_like(both))
        rows = slice(block * step, (block + 1) * step)
        raw = jnp.dot(
            k_ref[rows, pair * 2 * head : (pair + 1) * 2 * head],
            mine,
            preferred_element_type=jnp.float32,
        )
        raw = raw + bias_ref[rows, :]
        score_ref[h % 2, rows, :] = raw
        return jnp.maximum(top, jnp.max(raw.reshape(step // 8, 8, span), axis=0))

    def weighted(h, block, top, total):
        rows = slice(block * step, (block + 1) * step)
        prob = jnp.exp2((score_ref[h % 2, rows, :] - top) * factor).astype(jnp.bfloat16)
        term = jnp.dot(
            v_ref[h * v_rows : (h + 1) * v_rows, rows], prob, preferred_element_type=jnp.float32
        )
        return term if total is None else total + term

    def finish(h, top, total):
        peak = top * scale
        den = total[head : head + 1, :] + jnp.exp(-peak)
        part_ref[h * head : (h + 1) * head, :] = (total[:head, :] / den).astype(jnp.bfloat16)
        stat_ref[h : h + 1, :] = peak
        stat_ref[HEADS + h : HEADS + h + 1, :] = den

    zero = jnp.zeros((8, span), jnp.float32)
    tops = zero
    for block in range(blocks):
        tops = scores(0, block, tops)
    for h in range(HEADS):
        top = jnp.max(tops, axis=0, keepdims=True)
        total, tops = None, zero
        for block in range(blocks):
            if h + 1 < HEADS:
                tops = scores(h + 1, block, tops)
            total = weighted(h, block, top, total)
        finish(h, top, total)


MESH = pl.DeviceIdType.MESH
GROUPS = 4
STEPS = 2 * GROUPS
FINAL = ((0, 3), (0, 2), (0, 1), (1, 3), (1, 2), (0, 0), (1, 1), (1, 0))


def pick(values, index):
    out = values[0]
    for n, value in enumerate(values[1:]):
        out = jnp.where(index == n + 1, value, out)
    return out


def fused_kernel(
    rows,
    cols,
    table_ref,
    masks_ref,
    features_ref,
    wq_ref,
    wk_ref,
    wv_ref,
    out_ref,
    kf,
    qf,
    wq_t,
    wv_t,
    words_out,
    words,
    k_all,
    v_all,
    q_all,
    part,
    stat,
    mate_part,
    mate_stat,
    both_part,
    both_stat,
    fin_part,
    fin_stat,
    bias,
    score,
    q_send,
    q_recv,
    z_send,
    z_recv,
    row_send,
    row_recv,
    word_send,
    word_recv,
    pair_send,
    pair_recv,
    fin_send,
    fin_recv,
):
    nodes, width = features_ref.shape
    head = width // HEADS
    f32 = jnp.float32
    chips = cols // 2
    planes = chips // 2
    last = planes - 1
    turns = planes * STEPS
    tiles = nodes // TILE
    square = rows == 4
    r, c = lax.axis_index("row"), lax.axis_index("col")
    m, k = c // 2, lax.rem(c, 2)
    other = m + 1 - 2 * lax.rem(m, 2)
    mate = (r, m * 2 + 1 - k)
    partner = (r, other * 2 + k)

    def reader(j):
        return lax.rem(m + chips - 2 * j, chips)

    def flip(place, b):
        return place + 1 - 2 * lax.rem(place, 2) if b else place

    def row_to(d):
        if rows % 2:
            return lax.rem(r + d, rows)
        return flip(lax.rem(r + d // 2 * 2, rows), d % 2)

    def row_from(d):
        if rows % 2:
            return lax.rem(r + rows - d, rows)
        return lax.rem(flip(r, d % 2) + rows - d // 2 * 2, rows)

    def send(src, dst, send_sem, recv_sem, device):
        return pltpu.make_async_remote_copy(
            src_ref=src,
            dst_ref=dst,
            send_sem=send_sem,
            recv_sem=recv_sem,
            device_id=device,
            device_id_type=MESH,
        )

    barrier = pltpu.get_barrier_semaphore()
    peers = [mate, partner]
    peers += [(lax.rem(r + d, rows), c) for d in range(1, rows)]
    peers += [(r, reader(j) * 2 + k) for j in range(1, planes)]
    for peer in peers:
        pl.semaphore_signal(barrier, inc=1, device_id=peer, device_id_type=MESH)
    pl.semaphore_wait(barrier, len(peers))

    def query_copy(step):
        if step == 0:
            return send(features_ref, qf.at[1], q_send.at[0], q_recv.at[1], mate)
        if step == 1:
            return send(features_ref, qf.at[2], q_send.at[1], q_recv.at[2], partner)
        return send(qf.at[2], qf.at[3], q_send.at[2], q_recv.at[3], mate)

    def line_copy(j, tile):
        span = pl.ds(tile * TILE, TILE)
        return send(
            features_ref.at[span],
            kf.at[j, r, span],
            z_send.at[j, tile],
            z_recv.at[j, tile],
            (r, reader(j) * 2 + k),
        )

    def pieces(j, unit):
        if j == 0:
            return (0, TILE, 0), (TILE, TILE, 1)
        half = TILE // 2
        return (unit * TILE, half, 2 * unit), (unit * TILE + half, half, 2 * unit + 1)

    def row_copy(j, row, d, piece, own=False):
        start, size, n = piece
        span = pl.ds(start, size)
        return send(
            features_ref.at[span] if own else kf.at[j, row, span],
            kf.at[j, row, span],
            row_send.at[j, row, d, n],
            row_recv.at[j, row, n],
            (row_to(d), c),
        )

    def spread_copies(j, unit):
        low, high = pieces(j, unit)
        own = j == 0
        if square:
            order = [(1, high), (2, low), (1, low), (2, high)]
        else:
            order = [(d, piece) for piece in (low, high) for d in range(1, rows)]
        return [row_copy(j, r, d, piece, own) for d, piece in order]

    def relay_copies(j, unit):
        if not square:
            return []
        low, high = pieces(j, unit)
        return [row_copy(j, row_from(1), 2, high), row_copy(j, row_from(2), 1, low)]

    def await_piece(j, d, piece):
        row_copy(j, row_from(d), 1, piece).wait_recv()

    def relay(j, unit):
        low, high = pieces(j, unit)
        for copy, d, piece in zip(relay_copies(j, unit), (1, 2), (high, low)):
            await_piece(j, d, piece)
            copy.start()

    def late_pieces(j, half):
        if j == 0:
            low, high = pieces(0, 0)
            if square:
                return [] if half == 0 else [(1, low), (2, high), (3, low), (3, high)]
            span = range(1, rows // 2) if half == 0 else range(rows // 2, rows)
            return [(d, piece) for d in span for piece in (low, high)]
        low, high = pieces(j, half)
        if square:
            return [(1, low), (2, high), (3, low), (3, high)]
        return [(d, piece) for d in range(1, rows) for piece in (low, high)]

    def order(j, half):
        if j == 0:
            if square:
                return [(0, 0), (0, 1), (1, 1), (2, 0)] if half == 0 else [(1, 0), (2, 1), (3, 0), (3, 1)]
            span = range(rows // 2) if half == 0 else range(rows // 2, rows)
            return [(d, t) for d in span for t in range(tiles)]
        return [(d, half) for d in range(rows)]

    def word_copy(j):
        return send(
            words_out.at[j - 1],
            words.at[j],
            word_send.at[j],
            word_recv.at[j],
            (r, reader(j) * 2 + k),
        )

    query_copy(1).start()
    for j in range(1, planes):
        for tile in range(tiles):
            line_copy(j, tile).start()
    for copy in spread_copies(0, 0):
        copy.start()
    query_copy(0).start()

    k_tiles = rows * tiles
    entries = 2 * 2 * tiles * k_tiles

    def gather_words(j, dst):
        first = reader(j) // 2 * entries

        def step(s, carry):
            for u in range(8):
                e = s * 8 + u
                entry = table_ref[first + e]
                dst[e] = masks_ref[jnp.maximum(entry, 0)] * jnp.where(entry >= 0, 1, 0)
            return carry

        lax.fori_loop(0, entries // 8, step, 0)

    for j in range(1, planes):
        gather_words(j, words_out.at[j - 1])
        word_copy(j).start()

    kf[0, r] = features_ref[...]
    qf[0] = features_ref[...]
    wq_t[...] = wq_ref[...].T
    wv_t[...] = wv_ref[...].T
    half_keys = rows * nodes // 2
    for n in range(2 * planes):
        for h in range(HEADS):
            v_all[n, h * (head + ONES) + head : (h + 1) * (head + ONES), :] = jnp.ones(
                (ONES, half_keys), jnp.bfloat16
            )
    gather_words(0, words.at[0])

    def project(j, half, spot):
        block = jnp.concatenate(
            [
                kf[j, row_from(d), t * TILE : (t + 1) * TILE, :]
                for d, t in order(j, half)[spot : spot + 2]
            ],
            axis=0,
        )
        n = 2 * j + half
        lane = slice(spot * TILE, (spot + 2) * TILE)
        k_all[n, lane, :] = jnp.dot(block, wk_ref[...], preferred_element_type=f32).astype(
            jnp.bfloat16
        )
        value = lax.dot_general(
            wv_t[...], block, (((1,), (1,)), ((), ())), preferred_element_type=f32
        ).astype(jnp.bfloat16)
        for h in range(HEADS):
            v_all[n, h * (head + ONES) : h * (head + ONES) + head, lane] = value[
                h * head : (h + 1) * head, :
            ]

    def begin(j, half):
        for d, piece in late_pieces(j, half):
            await_piece(j, d, piece)
        for spot in range(2 if (j, half) == (0, 0) else 0, rows * tiles // 2, 2):
            project(j, half, spot)
        if j > 0 and half == 0:
            word_copy(j).wait_recv()

    def pair_copies(i, n, which):
        return (
            send(
                part.at[i],
                mate_part.at[n, which],
                pair_send.at[n, which, 0],
                pair_recv.at[n, which, 0],
                mate,
            ),
            send(
                stat.at[i],
                mate_stat.at[n, which],
                pair_send.at[n, which, 1],
                pair_recv.at[n, which, 1],
                mate,
            ),
        )

    fin_copies = (
        send(both_part, fin_part, fin_send.at[0], fin_recv.at[0], partner),
        send(both_stat, fin_stat, fin_send.at[1], fin_recv.at[1], partner),
    )

    def weigh(sources):
        peaks = [ref[0:HEADS, :] for _, ref in sources]
        top = functools.reduce(jnp.maximum, peaks)
        weights = [
            jnp.exp(peak - top) * ref[HEADS : 2 * HEADS, :]
            for peak, (_, ref) in zip(peaks, sources)
        ]
        total = functools.reduce(jnp.add, weights)
        return top, weights, total

    def blend(sources, weights, total, h):
        rows_of = slice(h * head, (h + 1) * head)
        numer = functools.reduce(
            jnp.add,
            [
                ref[rows_of, :].astype(f32) * weight[h : h + 1, :]
                for weight, (ref, _) in zip(weights, sources)
            ],
        )
        return (numer / total[h : h + 1, :]).astype(jnp.bfloat16)

    def turn_of(j, half, slot):
        if j < last:
            return j * STEPS + half * GROUPS + slot
        return j * STEPS + FINAL.index((half, slot))

    def gathered(which):
        sources = []
        for j in range(planes):
            for half in range(2):
                n = 2 * j + half
                for copy in pair_copies(0, n, which):
                    copy.wait_recv()
                i = turn_of(j, half, 2 * which)
                sources.append((part.at[i], stat.at[i]))
                sources.append((mate_part.at[n, which], mate_stat.at[n, which]))
        return sources

    project(0, 0, 0)
    relay(0, 0)

    def turn(i, carry):
        j = i // STEPS
        u = lax.rem(i, STEPS)
        ending = j == last
        half = jnp.where(ending, pick([a for a, _ in FINAL], u), u // GROUPS)
        slot = jnp.where(ending, pick([b for _, b in FINAL], u), lax.rem(u, GROUPS))
        n = 2 * j + half
        chip = jnp.where(slot < 2, m, other)
        lane = jnp.where(lax.rem(slot, 2) == 0, k, 1 - k)
        first = (lax.rem(chip, 2) * 2 + lane) * tiles * k_tiles

        for plane in range(1, planes):
            base = (plane - 1) * STEPS
            for unit in range(tiles):

                @pl.when(i == base + 4 * unit + 2)
                def _():
                    line_copy(plane, unit).wait_recv()
                    for copy in spread_copies(plane, unit):
                        copy.start()

                @pl.when(i == base + 4 * unit + 4)
                def _():
                    relay(plane, unit)

        @pl.when(i == min(2, last * 2))
        def _():
            query_copy(1).wait_recv()
            query_copy(2).start()

        for plane in range(planes):
            for part_of in range(2):
                if plane < last:
                    at = plane * STEPS + part_of * GROUPS
                else:
                    at = plane * STEPS + 3 * part_of

                @pl.when(i == at)
                def _():
                    begin(plane, part_of)

        fresh = (j == 0) & (half == 0)

        @pl.when(fresh & (lax.rem(slot, 2) == 1))
        def _():
            send(qf.at[slot], qf.at[slot], q_send.at[0], q_recv.at[slot], mate).wait_recv()

        @pl.when(fresh)
        def _():
            q_all[slot] = lax.dot_general(
                wq_t[...], qf[slot], (((1,), (1,)), ((), ())), preferred_element_type=f32
            ).astype(jnp.bfloat16)

        spots = []
        for spot in range(rows * tiles // 2):
            choices = [order(0, 0)[spot], order(0, 1)[spot], order(1, 0)[spot], order(1, 1)[spot]]
            index = [row_from(d) * tiles + t for d, t in choices]
            spots.append(
                jnp.where(
                    j == 0,
                    jnp.where(half == 0, index[0], index[1]),
                    jnp.where(half == 0, index[2], index[3]),
                )
            )
        build_bias(words.at[j], first, k_tiles, spots, bias)

        @pl.when(i == last * STEPS + 5)
        def _():
            sources = gathered(1)
            top, weights, total = weigh(sources)
            both_stat[0:HEADS, :] = top
            both_stat[HEADS : 2 * HEADS, :] = total
            for h in range(HEADS):
                both_part[h * head : (h + 1) * head, :] = blend(sources, weights, total, h)
            for copy in fin_copies:
                copy.start()

        attend_group(
            q_all.at[slot], k_all.at[n], v_all.at[n], part.at[i], stat.at[i], bias, score
        )

        @pl.when(lax.rem(slot, 2) == 1)
        def _():
            for copy in pair_copies(i, n, slot // 2):
                copy.start()

        return carry

    lax.fori_loop(0, turns, turn, 0)

    sources = gathered(0)
    for copy in fin_copies:
        copy.wait_recv()
    sources.append((fin_part, fin_stat))
    _, weights, total = weigh(sources)
    for h in range(HEADS):
        out_ref[h * head : (h + 1) * head, :] = blend(sources, weights, total, h)

    for step in range(3):
        query_copy(step).wait_send()
    for j in range(planes):
        for unit in range(tiles if j else 1):
            for copy in spread_copies(j, unit) + relay_copies(j, unit):
                copy.wait_send()
        if j:
            for tile in range(tiles):
                line_copy(j, tile).wait_send()
            word_copy(j).wait_send()
    for n in range(2 * planes):
        for which in range(2):
            for copy in pair_copies(0, n, which):
                copy.wait_send()
    for copy in fin_copies:
        copy.wait_send()


def fused(mesh_shape, table, masks, features, w_query, w_key, w_value):
    rows, cols = mesh_shape["row"], mesh_shape["col"]
    planes = cols // 4
    turns = planes * STEPS
    nodes, width = features.shape
    keys = rows * nodes // 2
    head = width // HEADS
    tiles = nodes // TILE
    entries = 2 * 2 * tiles * rows * tiles
    bf16, f32, i32 = jnp.bfloat16, jnp.float32, jnp.int32
    whole = pl.BlockSpec(memory_space=pltpu.VMEM)
    dma = pltpu.SemaphoreType.DMA
    return pl.pallas_call(
        functools.partial(fused_kernel, rows, cols),
        out_shape=jax.ShapeDtypeStruct((width, nodes), bf16),
        in_specs=[pl.BlockSpec(memory_space=pltpu.SMEM)] + [whole] * 5,
        out_specs=whole,
        scratch_shapes=[
            pltpu.VMEM((planes, rows, nodes, width), bf16),
            pltpu.VMEM((GROUPS, nodes, width), bf16),
            pltpu.VMEM((width, width), bf16),
            pltpu.VMEM((width, width), bf16),
            pltpu.VMEM((max(planes - 1, 1), entries, TILE // 32, TILE), i32),
            pltpu.VMEM((planes, entries, TILE // 32, TILE), i32),
            pltpu.VMEM((2 * planes, keys, width), bf16),
            pltpu.VMEM((2 * planes, HEADS * (head + ONES), keys), bf16),
            pltpu.VMEM((GROUPS, width, nodes), bf16),
            pltpu.VMEM((turns, width, nodes), bf16),
            pltpu.VMEM((turns, 2 * HEADS, nodes), f32),
            pltpu.VMEM((2 * planes, 2, width, nodes), bf16),
            pltpu.VMEM((2 * planes, 2, 2 * HEADS, nodes), f32),
            pltpu.VMEM((width, nodes), bf16),
            pltpu.VMEM((2 * HEADS, nodes), f32),
            pltpu.VMEM((width, nodes), bf16),
            pltpu.VMEM((2 * HEADS, nodes), f32),
            pltpu.VMEM((keys, nodes), f32),
            pltpu.VMEM((2, keys, nodes), f32),
            dma((3,)),
            dma((GROUPS,)),
            dma((planes, tiles)),
            dma((planes, tiles)),
            dma((planes, rows, rows, 2 * tiles)),
            dma((planes, rows, 2 * tiles)),
            dma((planes,)),
            dma((planes,)),
            dma((2 * planes, 2, 2)),
            dma((2 * planes, 2, 2)),
            dma((2,)),
            dma((2,)),
        ],
        compiler_params=pltpu.CompilerParams(
            collective_id=0, has_side_effects=True, vmem_limit_bytes=60 * 1024 * 1024
        ),
        name="fused",
    )(table, masks, features, w_query, w_key, w_value)


def entry_table(pairs, count, q_tiles, k_tiles):
    entries = pairs.shape[0]
    ids = lax.broadcasted_iota(jnp.int32, (q_tiles * k_tiles, entries), 1)
    cell = lax.broadcasted_iota(jnp.int32, (q_tiles * k_tiles, entries), 0)
    code = (pairs[:, 0] * k_tiles + pairs[:, 1])[None, :]
    return jnp.max(jnp.where((code == cell) & (ids < count), ids, -1), axis=1)


def body(mesh_shape, features, w_query, w_key, w_value, w_out, pairs, counts, masks):
    nodes = features.shape[0]
    rows, cols = mesh_shape["row"], mesh_shape["col"]
    table = entry_table(pairs[0, 0], counts[0, 0], cols * nodes // TILE, rows * nodes // TILE)
    words = masks[0, 0].transpose(0, 2, 1)
    attended = fused(mesh_shape, table, words, features, w_query, w_key, w_value)
    return lax.dot_general(
        attended, w_out, (((0,), (0,)), ((), ())), preferred_element_type=jnp.float32
    ).astype(jnp.bfloat16)


def solution(mesh):
    in_specs = (
        P(("row", "col"), None),
        P(),
        P(),
        P(),
        P(),
        P("row", "col", None, None),
        P("row", "col"),
        P("row", "col", None, None, None),
    )
    out_specs = P(("row", "col"), None)
    return jax.shard_map(
        functools.partial(body, dict(mesh.shape)), mesh=mesh, in_specs=in_specs, out_specs=out_specs, check_vma=False)
```

```python
import functools
import math

import jax
import jax.numpy as jnp
from jax import lax
from jax.experimental import pallas as pl
from jax.experimental.pallas import tpu as pltpu
from jax.sharding import PartitionSpec as P

HEADS = 8
TILE = 128
BLOCK = 256
ONES = 16
MESH = pl.DeviceIdType.MESH
STEPS = 4
FINAL = ((0, 1), (1, 1), (0, 0), (1, 0))


def build_bias(words_ref, first, k_tiles, spots, bias_ref):
    span = bias_ref.shape[1]
    tiles = span // TILE
    shift = 31 - lax.broadcasted_iota(jnp.int32, (32, TILE), 0)
    for b, spot in enumerate(spots):
        for t in range(tiles):
            words = words_ref[first + t * k_tiles + spot]
            for j in range(TILE // 32):
                bits = jnp.broadcast_to(words[j : j + 1, :], (32, TILE)) << shift
                bias_ref[pl.ds(b * TILE + j * 32, 32), pl.ds(t * TILE, TILE)] = jnp.where(
                    bits < 0, 0.0, -jnp.inf
                )


def attend(q_ref, k_ref, v_ref, part_ref, stat_ref, bias_ref, score_ref):
    heads, keys, _ = k_ref.shape
    span = q_ref.shape[3]
    head = v_ref.shape[1] - ONES
    blocks = keys // BLOCK
    zero = jnp.zeros((8, span), jnp.float32)

    def scores(h, s, block, top):
        rows = slice(block * BLOCK, (block + 1) * BLOCK)
        raw = jnp.dot(k_ref[h, rows, :], q_ref[s, h], preferred_element_type=jnp.float32)
        raw = raw + bias_ref[s, rows, :]
        score_ref[h % 2, s, rows, :] = raw
        return jnp.maximum(top, jnp.max(raw.reshape(BLOCK // 8, 8, span), axis=0))

    def weighted(h, s, block, top, total):
        rows = slice(block * BLOCK, (block + 1) * BLOCK)
        prob = jnp.exp2(score_ref[h % 2, s, rows, :] - top).astype(jnp.bfloat16)
        term = jnp.dot(v_ref[h, :, rows], prob, preferred_element_type=jnp.float32)
        return term if total is None else total + term

    def finish(h, s, top, total):
        den = total[head : head + 1, :] + jnp.exp2(-top)
        part_ref[s, h * head : (h + 1) * head, :] = (total[:head, :] / den).astype(jnp.bfloat16)
        stat_ref[s, h : h + 1, :] = top
        stat_ref[s, heads + h : heads + h + 1, :] = den

    tops = [zero, zero]
    for s in range(2):
        for block in range(blocks):
            tops[s] = scores(0, s, block, tops[s])
    for h in range(heads):
        later = [zero, zero]
        for s in range(2):
            top = jnp.max(tops[s], axis=0, keepdims=True)
            total = None
            for block in range(blocks):
                if h + 1 < heads:
                    later[s] = scores(h + 1, s, block, later[s])
                total = weighted(h, s, block, top, total)
            finish(h, s, top, total)
        tops = later


def pick(values, index):
    out = values[0]
    for n, value in enumerate(values[1:]):
        out = jnp.where(index == n + 1, value, out)
    return out


def fused_kernel(
    rows,
    cols,
    table_ref,
    masks_ref,
    features_ref,
    wq_ref,
    wk_ref,
    wv_ref,
    out_ref,
    kf,
    qf,
    wq_t,
    wv_t,
    words_out,
    words,
    k_all,
    v_all,
    q_all,
    part,
    stat,
    mate_part,
    mate_stat,
    both_part,
    both_stat,
    fin_part,
    fin_stat,
    numer,
    bias,
    score,
    q_send,
    q_recv,
    z_send,
    z_recv,
    row_send,
    row_recv,
    word_send,
    word_recv,
    pair_send,
    pair_recv,
    fin_send,
    fin_recv,
):
    nodes, width = features_ref.shape
    head = width // HEADS
    f32 = jnp.float32
    chips = cols // 2
    planes = chips // 2
    last = planes - 1
    turns = planes * STEPS
    tiles = nodes // TILE
    square = rows == 4
    r, c = lax.axis_index("row"), lax.axis_index("col")
    m, k = c // 2, lax.rem(c, 2)
    other = m + 1 - 2 * lax.rem(m, 2)
    mate = (r, m * 2 + 1 - k)
    partner = (r, other * 2 + k)

    def reader(j):
        return lax.rem(m + chips - 2 * j, chips)

    def flip(place, b):
        return place + 1 - 2 * lax.rem(place, 2) if b else place

    def row_to(d):
        if rows % 2:
            return lax.rem(r + d, rows)
        return flip(lax.rem(r + d // 2 * 2, rows), d % 2)

    def row_from(d):
        if rows % 2:
            return lax.rem(r + rows - d, rows)
        return lax.rem(flip(r, d % 2) + rows - d // 2 * 2, rows)

    def send(src, dst, send_sem, recv_sem, device):
        return pltpu.make_async_remote_copy(
            src_ref=src,
            dst_ref=dst,
            send_sem=send_sem,
            recv_sem=recv_sem,
            device_id=device,
            device_id_type=MESH,
        )

    barrier = pltpu.get_barrier_semaphore()
    peers = [mate, partner]
    peers += [(lax.rem(r + d, rows), c) for d in range(1, rows)]
    peers += [(r, reader(j) * 2 + k) for j in range(1, planes)]
    for peer in peers:
        pl.semaphore_signal(barrier, inc=1, device_id=peer, device_id_type=MESH)
    pl.semaphore_wait(barrier, len(peers))

    def query_copy(step):
        if step == 0:
            return send(features_ref, qf.at[1], q_send.at[0], q_recv.at[1], mate)
        if step == 1:
            return send(features_ref, qf.at[2], q_send.at[1], q_recv.at[2], partner)
        return send(qf.at[2], qf.at[3], q_send.at[2], q_recv.at[3], mate)

    def line_copy(j, tile):
        span = pl.ds(tile * TILE, TILE)
        return send(
            features_ref.at[span],
            kf.at[j, r, span],
            z_send.at[j, tile],
            z_recv.at[j, tile],
            (r, reader(j) * 2 + k),
        )

    def pieces(j, unit):
        if j == 0:
            return (0, TILE, 0), (TILE, TILE, 1)
        half = TILE // 2
        return (unit * TILE, half, 2 * unit), (unit * TILE + half, half, 2 * unit + 1)

    def row_copy(j, row, d, piece, own=False):
        start, size, n = piece
        span = pl.ds(start, size)
        return send(
            features_ref.at[span] if own else kf.at[j, row, span],
            kf.at[j, row, span],
            row_send.at[j, row, d, n],
            row_recv.at[j, row, n],
            (row_to(d), c),
        )

    def spread_copies(j, unit):
        low, high = pieces(j, unit)
        own = j == 0
        if square:
            order = [(1, high), (2, low), (1, low), (2, high)]
        else:
            order = [(d, piece) for piece in (low, high) for d in range(1, rows)]
        return [row_copy(j, r, d, piece, own) for d, piece in order]

    def relay_copies(j, unit):
        if not square:
            return []
        low, high = pieces(j, unit)
        return [row_copy(j, row_from(1), 2, high), row_copy(j, row_from(2), 1, low)]

    def await_piece(j, d, piece):
        row_copy(j, row_from(d), 1, piece).wait_recv()

    def relay(j, unit):
        low, high = pieces(j, unit)
        for copy, d, piece in zip(relay_copies(j, unit), (1, 2), (high, low)):
            await_piece(j, d, piece)
            copy.start()

    def late_pieces(j, half):
        if j == 0:
            low, high = pieces(0, 0)
            if square:
                return [] if half == 0 else [(1, low), (2, high), (3, low), (3, high)]
            span = range(1, rows // 2) if half == 0 else range(rows // 2, rows)
            return [(d, piece) for d in span for piece in (low, high)]
        low, high = pieces(j, half)
        if square:
            return [(1, low), (2, high), (3, low), (3, high)]
        return [(d, piece) for d in range(1, rows) for piece in (low, high)]

    def order(j, half):
        if j == 0:
            if square:
                return [(0, 0), (0, 1), (1, 1), (2, 0)] if half == 0 else [(1, 0), (2, 1), (3, 0), (3, 1)]
            span = range(rows // 2) if half == 0 else range(rows // 2, rows)
            return [(d, t) for d in span for t in range(tiles)]
        return [(d, half) for d in range(rows)]

    def word_copy(j):
        return send(
            words_out.at[j - 1],
            words.at[j],
            word_send.at[j],
            word_recv.at[j],
            (r, reader(j) * 2 + k),
        )

    query_copy(1).start()
    for j in range(1, planes):
        for tile in range(tiles):
            line_copy(j, tile).start()
    for copy in spread_copies(0, 0):
        copy.start()
    query_copy(0).start()

    k_tiles = rows * tiles
    entries = 2 * 2 * tiles * k_tiles

    def gather_words(j, dst):
        first = reader(j) // 2 * entries

        def step(s, carry):
            for u in range(8):
                e = s * 8 + u
                entry = table_ref[first + e]
                dst[e] = masks_ref[jnp.maximum(entry, 0)] * jnp.where(entry >= 0, 1, 0)
            return carry

        lax.fori_loop(0, entries // 8, step, 0)

    for j in range(1, planes):
        gather_words(j, words_out.at[j - 1])
        word_copy(j).start()

    kf[0, r] = features_ref[...]
    qf[0] = features_ref[...]
    wq_t[...] = wq_ref[...].T
    wv_t[...] = wv_ref[...].T
    half_keys = rows * nodes // 2
    for n in range(2 * planes):
        v_all[n, :, head : head + ONES, :] = jnp.ones((HEADS, ONES, half_keys), jnp.bfloat16)
    gather_words(0, words.at[0])

    def project(j, half, spot):
        block = jnp.concatenate(
            [
                kf[j, row_from(d), t * TILE : (t + 1) * TILE, :]
                for d, t in order(j, half)[spot : spot + 2]
            ],
            axis=0,
        )
        n = 2 * j + half
        lane = slice(spot * TILE, (spot + 2) * TILE)
        key = jnp.dot(block, wk_ref[...], preferred_element_type=f32)
        left = lax.broadcasted_iota(jnp.int32, (2 * TILE, 2 * head), 1) < head
        for p in range(HEADS // 2):
            both = key[:, p * 2 * head : (p + 1) * 2 * head]
            turned = pltpu.roll(both, head, 1)
            k_all[n, 2 * p, lane, :] = jnp.where(left, both, turned).astype(jnp.bfloat16)
            k_all[n, 2 * p + 1, lane, :] = jnp.where(left, turned, both).astype(jnp.bfloat16)
        value = lax.dot_general(
            wv_t[...], block, (((1,), (1,)), ((), ())), preferred_element_type=f32
        ).astype(jnp.bfloat16)
        for h in range(HEADS):
            v_all[n, h, :head, lane] = value[h * head : (h + 1) * head, :]

    def begin(j, half):
        for d, piece in late_pieces(j, half):
            await_piece(j, d, piece)
        for spot in range(2 if (j, half) == (0, 0) else 0, rows * tiles // 2, 2):
            project(j, half, spot)
        if j > 0 and half == 0:
            word_copy(j).wait_recv()

    def pair_copies(i, n, which):
        return (
            send(
                part.at[i, 1],
                mate_part.at[n, which],
                pair_send.at[n, which, 0],
                pair_recv.at[n, which, 0],
                mate,
            ),
            send(
                stat.at[i, 1],
                mate_stat.at[n, which],
                pair_send.at[n, which, 1],
                pair_recv.at[n, which, 1],
                mate,
            ),
        )

    fin_copies = (
        send(both_part, fin_part, fin_send.at[0], fin_recv.at[0], partner),
        send(both_stat, fin_stat, fin_send.at[1], fin_recv.at[1], partner),
    )

    def weigh(sources):
        peaks = [ref[0:HEADS, :] for _, ref in sources]
        top = functools.reduce(jnp.maximum, peaks)
        weights = [
            jnp.exp2(peak - top) * ref[HEADS : 2 * HEADS, :]
            for peak, (_, ref) in zip(peaks, sources)
        ]
        total = functools.reduce(jnp.add, weights)
        return top, weights, total

    def mixed(sources, weights, h):
        rows_of = slice(h * head, (h + 1) * head)
        return functools.reduce(
            jnp.add,
            [
                ref[rows_of, :].astype(f32) * weight[h : h + 1, :]
                for weight, (ref, _) in zip(weights, sources)
            ],
        )

    def turn_of(j, half, which):
        if j < last:
            return j * STEPS + half * 2 + which
        return j * STEPS + FINAL.index((half, which))

    def gathered(which):
        sources = []
        for j in range(planes):
            for half in range(2):
                n = 2 * j + half
                for copy in pair_copies(0, n, which):
                    copy.wait_recv()
                i = turn_of(j, half, which)
                sources.append((part.at[i, 0], stat.at[i, 0]))
                sources.append((mate_part.at[n, which], mate_stat.at[n, which]))
        return sources

    project(0, 0, 0)
    relay(0, 0)

    factor = math.log2(math.e) / math.sqrt(head)

    def queries(which, s):
        value = lax.dot_general(
            wq_t[...], qf[2 * which + s], (((1,), (1,)), ((), ())), preferred_element_type=f32
        )
        value = value.astype(jnp.bfloat16).astype(f32) * factor
        high = value.astype(jnp.bfloat16)
        low = (value - high.astype(f32)).astype(jnp.bfloat16)
        for h in range(HEADS):
            rows_of = slice(h * head, (h + 1) * head)
            q_all[which, s, h, :head, :] = high[rows_of, :]
            q_all[which, s, h, head:, :] = low[rows_of, :]

    def await_query(slot):
        send(qf.at[slot], qf.at[slot], q_send.at[0], q_recv.at[slot], mate).wait_recv()

    def turn(i, carry):
        j = i // STEPS
        u = lax.rem(i, STEPS)
        ending = j == last
        half = jnp.where(ending, pick([a for a, _ in FINAL], u), u // 2)
        which = jnp.where(ending, pick([b for _, b in FINAL], u), lax.rem(u, 2))
        n = 2 * j + half
        chip = jnp.where(which == 0, m, other)

        @pl.when(i == turn_of(0, 0, 1))
        def _():
            query_copy(1).wait_recv()
            query_copy(2).start()

        for plane in range(1, planes):
            base = (plane - 1) * STEPS
            for unit in range(tiles):

                @pl.when(i == base + 2 * unit + 1)
                def _():
                    line_copy(plane, unit).wait_recv()
                    for copy in spread_copies(plane, unit):
                        copy.start()

                @pl.when(i == base + 2 * unit + 2)
                def _():
                    relay(plane, unit)

        for plane in range(planes):
            for part_of in range(2):

                @pl.when(i == min(turn_of(plane, part_of, 0), turn_of(plane, part_of, 1)))
                def _():
                    begin(plane, part_of)

        for pair in range(2):

            @pl.when(i == turn_of(0, 0, pair))
            def _():
                queries(pair, 0)
                await_query(2 * pair + 1)
                queries(pair, 1)

        @pl.when(i == last * STEPS + 2)
        def _():
            sources = gathered(1)
            top, weights, total = weigh(sources)
            both_stat[0:HEADS, :] = top
            both_stat[HEADS : 2 * HEADS, :] = total
            for h in range(HEADS):
                both_part[h * head : (h + 1) * head, :] = (
                    mixed(sources, weights, h) / total[h : h + 1, :]
                ).astype(jnp.bfloat16)
            for copy in fin_copies:
                copy.start()

        spots = []
        for spot in range(rows * tiles // 2):
            choices = [order(0, 0)[spot], order(0, 1)[spot], order(1, 0)[spot], order(1, 1)[spot]]
            index = [row_from(d) * tiles + t for d, t in choices]
            spots.append(
                jnp.where(
                    j == 0,
                    jnp.where(half == 0, index[0], index[1]),
                    jnp.where(half == 0, index[2], index[3]),
                )
            )
        for s in range(2):
            lane = k if s == 0 else 1 - k
            first = (lax.rem(chip, 2) * 2 + lane) * tiles * k_tiles
            build_bias(words.at[j], first, k_tiles, spots, bias.at[s])

        attend(q_all.at[which], k_all.at[n], v_all.at[n], part.at[i], stat.at[i], bias, score)

        for copy in pair_copies(i, n, which):
            copy.start()

        return carry

    lax.fori_loop(0, turns, turn, 0)

    sources = gathered(0)
    top, weights, total = weigh(sources)
    for h in range(HEADS):
        numer[h * head : (h + 1) * head, :] = mixed(sources, weights, h)
    for copy in fin_copies:
        copy.wait_recv()
    peak = jnp.maximum(top, fin_stat[0:HEADS, :])
    mine = jnp.exp2(top - peak)
    theirs = jnp.exp2(fin_stat[0:HEADS, :] - peak) * fin_stat[HEADS : 2 * HEADS, :]
    den = total * mine + theirs
    mine, theirs = mine / den, theirs / den
    for h in range(HEADS):
        rows_of = slice(h * head, (h + 1) * head)
        out_ref[rows_of, :] = (
            numer[rows_of, :] * mine[h : h + 1, :]
            + fin_part[rows_of, :].astype(f32) * theirs[h : h + 1, :]
        ).astype(jnp.bfloat16)

    for step in range(3):
        query_copy(step).wait_send()
    for j in range(planes):
        for unit in range(tiles if j else 1):
            for copy in spread_copies(j, unit) + relay_copies(j, unit):
                copy.wait_send()
        if j:
            for tile in range(tiles):
                line_copy(j, tile).wait_send()
            word_copy(j).wait_send()
    for n in range(2 * planes):
        for which in range(2):
            for copy in pair_copies(0, n, which):
                copy.wait_send()
    for copy in fin_copies:
        copy.wait_send()


def fused(mesh_shape, table, masks, features, w_query, w_key, w_value):
    rows, cols = mesh_shape["row"], mesh_shape["col"]
    planes = cols // 4
    turns = planes * STEPS
    nodes, width = features.shape
    keys = rows * nodes // 2
    head = width // HEADS
    tiles = nodes // TILE
    entries = 2 * 2 * tiles * rows * tiles
    bf16, f32, i32 = jnp.bfloat16, jnp.float32, jnp.int32
    whole = pl.BlockSpec(memory_space=pltpu.VMEM)
    dma = pltpu.SemaphoreType.DMA
    return pl.pallas_call(
        functools.partial(fused_kernel, rows, cols),
        out_shape=jax.ShapeDtypeStruct((width, nodes), bf16),
        in_specs=[pl.BlockSpec(memory_space=pltpu.SMEM)] + [whole] * 5,
        out_specs=whole,
        scratch_shapes=[
            pltpu.VMEM((planes, rows, nodes, width), bf16),
            pltpu.VMEM((4, nodes, width), bf16),
            pltpu.VMEM((width, width), bf16),
            pltpu.VMEM((width, width), bf16),
            pltpu.VMEM((max(planes - 1, 1), entries, TILE // 32, TILE), i32),
            pltpu.VMEM((planes, entries, TILE // 32, TILE), i32),
            pltpu.VMEM((2 * planes, HEADS, keys, 2 * head), bf16),
            pltpu.VMEM((2 * planes, HEADS, head + ONES, keys), bf16),
            pltpu.VMEM((2, 2, HEADS, 2 * head, nodes), bf16),
            pltpu.VMEM((turns, 2, width, nodes), bf16),
            pltpu.VMEM((turns, 2, 2 * HEADS, nodes), f32),
            pltpu.VMEM((2 * planes, 2, width, nodes), bf16),
            pltpu.VMEM((2 * planes, 2, 2 * HEADS, nodes), f32),
            pltpu.VMEM((width, nodes), bf16),
            pltpu.VMEM((2 * HEADS, nodes), f32),
            pltpu.VMEM((width, nodes), bf16),
            pltpu.VMEM((2 * HEADS, nodes), f32),
            pltpu.VMEM((width, nodes), f32),
            pltpu.VMEM((2, keys, nodes), f32),
            pltpu.VMEM((2, 2, keys, nodes), f32),
            dma((3,)),
            dma((4,)),
            dma((planes, tiles)),
            dma((planes, tiles)),
            dma((planes, rows, rows, 2 * tiles)),
            dma((planes, rows, 2 * tiles)),
            dma((planes,)),
            dma((planes,)),
            dma((2 * planes, 2, 2)),
            dma((2 * planes, 2, 2)),
            dma((2,)),
            dma((2,)),
        ],
        compiler_params=pltpu.CompilerParams(
            collective_id=0, has_side_effects=True, vmem_limit_bytes=63 * 1024 * 1024
        ),
        name="fused",
    )(table, masks, features, w_query, w_key, w_value)


def entry_table(pairs, count, q_tiles, k_tiles):
    entries = pairs.shape[0]
    ids = lax.broadcasted_iota(jnp.int32, (q_tiles * k_tiles, entries), 1)
    cell = lax.broadcasted_iota(jnp.int32, (q_tiles * k_tiles, entries), 0)
    code = (pairs[:, 0] * k_tiles + pairs[:, 1])[None, :]
    return jnp.max(jnp.where((code == cell) & (ids < count), ids, -1), axis=1)


def body(mesh_shape, features, w_query, w_key, w_value, w_out, pairs, counts, masks):
    nodes = features.shape[0]
    rows, cols = mesh_shape["row"], mesh_shape["col"]
    table = entry_table(pairs[0, 0], counts[0, 0], cols * nodes // TILE, rows * nodes // TILE)
    words = masks[0, 0].transpose(0, 2, 1)
    attended = fused(mesh_shape, table, words, features, w_query, w_key, w_value)
    return lax.dot_general(
        attended, w_out, (((0,), (0,)), ((), ())), preferred_element_type=jnp.float32
    ).astype(jnp.bfloat16)


def solution(mesh):
    in_specs = (
        P(("row", "col"), None),
        P(),
        P(),
        P(),
        P(),
        P("row", "col", None, None),
        P("row", "col"),
        P("row", "col", None, None, None),
    )
    out_specs = P(("row", "col"), None)
    return jax.shard_map(
        functools.partial(body, dict(mesh.shape)), mesh=mesh, in_specs=in_specs, out_specs=out_specs, check_vma=False)
```

```python
import functools
import math

import jax
import jax.numpy as jnp
from jax import lax
from jax.experimental import pallas as pl
from jax.experimental.pallas import tpu as pltpu
from jax.sharding import PartitionSpec as P

HEADS = 8
TILE = 128
BLOCK = 256
ONES = 16
MESH = pl.DeviceIdType.MESH
STEPS = 4
FINAL = ((0, 1), (1, 1), (0, 0), (1, 0))


def build_bias(words_ref, first, k_tiles, spots, bias_ref):
    span = bias_ref.shape[1]
    tiles = span // TILE
    shift = 31 - lax.broadcasted_iota(jnp.int32, (32, TILE), 0)
    for b, spot in enumerate(spots):
        for t in range(tiles):
            words = words_ref[first + t * k_tiles + spot]
            for j in range(TILE // 32):
                bits = jnp.broadcast_to(words[j : j + 1, :], (32, TILE)) << shift
                bias_ref[pl.ds(b * TILE + j * 32, 32), pl.ds(t * TILE, TILE)] = jnp.where(
                    bits < 0, 0.0, -jnp.inf
                )


def attend(q_ref, k_ref, v_ref, part_ref, stat_ref, bias_ref, score_ref):
    heads, keys, _ = k_ref.shape
    span = q_ref.shape[3]
    head = v_ref.shape[1] - ONES
    blocks = keys // BLOCK
    zero = jnp.zeros((8, span), jnp.float32)

    def scores(h, s, block, top):
        rows = slice(block * BLOCK, (block + 1) * BLOCK)
        raw = jnp.dot(k_ref[h, rows, :], q_ref[s, h], preferred_element_type=jnp.float32)
        raw = raw + bias_ref[s, rows, :]
        score_ref[h % 2, s, rows, :] = raw
        return jnp.maximum(top, jnp.max(raw.reshape(BLOCK // 8, 8, span), axis=0))

    def weighted(h, s, block, top, total):
        rows = slice(block * BLOCK, (block + 1) * BLOCK)
        prob = jnp.exp2(score_ref[h % 2, s, rows, :] - top).astype(jnp.bfloat16)
        term = jnp.dot(v_ref[h, :, rows], prob, preferred_element_type=jnp.float32)
        return term if total is None else total + term

    def finish(h, s, top, total):
        den = total[head : head + 1, :] + jnp.exp2(-top)
        part_ref[s, h * head : (h + 1) * head, :] = (total[:head, :] / den).astype(jnp.bfloat16)
        stat_ref[s, h : h + 1, :] = top
        stat_ref[s, heads + h : heads + h + 1, :] = den

    tops = [zero, zero]
    for s in range(2):
        for block in range(blocks):
            tops[s] = scores(0, s, block, tops[s])
    for h in range(heads):
        later = [zero, zero]
        for s in range(2):
            top = jnp.max(tops[s], axis=0, keepdims=True)
            total = None
            for block in range(blocks):
                if h + 1 < heads:
                    later[s] = scores(h + 1, s, block, later[s])
                total = weighted(h, s, block, top, total)
            finish(h, s, top, total)
        tops = later


def pick(values, index):
    out = values[0]
    for n, value in enumerate(values[1:]):
        out = jnp.where(index == n + 1, value, out)
    return out


def fused_kernel(
    rows,
    cols,
    table_ref,
    masks_hbm,
    features_ref,
    wq_hbm,
    wk_hbm,
    wv_hbm,
    wo_hbm,
    out_ref,
    masks_ref,
    wq_ref,
    wk_ref,
    wv_ref,
    wo_ref,
    kf,
    qf,
    wq_t,
    wv_t,
    words_out,
    words,
    k_all,
    v_all,
    q_all,
    part,
    stat,
    mate_part,
    mate_stat,
    both_part,
    both_stat,
    fin_part,
    fin_stat,
    numer,
    attended,
    bias,
    score,
    q_send,
    q_recv,
    z_send,
    z_recv,
    row_send,
    row_recv,
    word_send,
    word_recv,
    pair_send,
    pair_recv,
    fin_send,
    fin_recv,
    load,
):
    nodes, width = features_ref.shape
    head = width // HEADS
    f32 = jnp.float32
    chips = cols // 2
    planes = chips // 2
    last = planes - 1
    turns = planes * STEPS
    tiles = nodes // TILE
    square = rows == 4
    r, c = lax.axis_index("row"), lax.axis_index("col")
    m, k = c // 2, lax.rem(c, 2)
    other = m + 1 - 2 * lax.rem(m, 2)
    mate = (r, m * 2 + 1 - k)
    partner = (r, other * 2 + k)

    def reader(j):
        return lax.rem(m + chips - 2 * j, chips)

    def flip(place, b):
        return place + 1 - 2 * lax.rem(place, 2) if b else place

    def row_to(d):
        if rows % 2:
            return lax.rem(r + d, rows)
        return flip(lax.rem(r + d // 2 * 2, rows), d % 2)

    def row_from(d):
        if rows % 2:
            return lax.rem(r + rows - d, rows)
        return lax.rem(flip(r, d % 2) + rows - d // 2 * 2, rows)

    def send(src, dst, send_sem, recv_sem, device):
        return pltpu.make_async_remote_copy(
            src_ref=src,
            dst_ref=dst,
            send_sem=send_sem,
            recv_sem=recv_sem,
            device_id=device,
            device_id_type=MESH,
        )

    loads = [
        pltpu.make_async_copy(src, dst, load.at[n])
        for n, (src, dst) in enumerate(
            (
                (masks_hbm, masks_ref),
                (wk_hbm, wk_ref),
                (wv_hbm, wv_ref),
                (wq_hbm, wq_ref),
                (wo_hbm, wo_ref),
            )
        )
    ]
    barrier = pltpu.get_barrier_semaphore()
    peers = [mate, partner]
    peers += [(lax.rem(r + d, rows), c) for d in range(1, rows)]
    peers += [(r, reader(j) * 2 + k) for j in range(1, planes)]
    for peer in peers:
        pl.semaphore_signal(barrier, inc=1, device_id=peer, device_id_type=MESH)
    for copy in loads:
        copy.start()
    pl.semaphore_wait(barrier, len(peers))

    def query_copy(step):
        if step == 0:
            return send(features_ref, qf.at[1], q_send.at[0], q_recv.at[1], mate)
        if step == 1:
            return send(features_ref, qf.at[2], q_send.at[1], q_recv.at[2], partner)
        return send(qf.at[2], qf.at[3], q_send.at[2], q_recv.at[3], mate)

    def line_copy(j, tile):
        span = pl.ds(tile * TILE, TILE)
        return send(
            features_ref.at[span],
            kf.at[j, r, span],
            z_send.at[j, tile],
            z_recv.at[j, tile],
            (r, reader(j) * 2 + k),
        )

    def pieces(j, unit):
        if j == 0:
            return (0, TILE, 0), (TILE, TILE, 1)
        half = TILE // 2
        return (unit * TILE, half, 2 * unit), (unit * TILE + half, half, 2 * unit + 1)

    def row_copy(j, row, d, piece, own=False):
        start, size, n = piece
        span = pl.ds(start, size)
        return send(
            features_ref.at[span] if own else kf.at[j, row, span],
            kf.at[j, row, span],
            row_send.at[j, row, d, n],
            row_recv.at[j, row, n],
            (row_to(d), c),
        )

    def spread_copies(j, unit):
        low, high = pieces(j, unit)
        own = j == 0
        if square:
            order = [(1, high), (2, low), (1, low), (2, high)]
        else:
            order = [(d, piece) for piece in (low, high) for d in range(1, rows)]
        return [row_copy(j, r, d, piece, own) for d, piece in order]

    def relay_copies(j, unit):
        if not square:
            return []
        low, high = pieces(j, unit)
        return [row_copy(j, row_from(1), 2, high), row_copy(j, row_from(2), 1, low)]

    def await_piece(j, d, piece):
        row_copy(j, row_from(d), 1, piece).wait_recv()

    def relay(j, unit):
        low, high = pieces(j, unit)
        for copy, d, piece in zip(relay_copies(j, unit), (1, 2), (high, low)):
            await_piece(j, d, piece)
            copy.start()

    def late_pieces(j, half):
        if j == 0:
            low, high = pieces(0, 0)
            if square:
                return [] if half == 0 else [(1, low), (2, high), (3, low), (3, high)]
            span = range(1, rows // 2) if half == 0 else range(rows // 2, rows)
            return [(d, piece) for d in span for piece in (low, high)]
        low, high = pieces(j, half)
        if square:
            return [(1, low), (2, high), (3, low), (3, high)]
        return [(d, piece) for d in range(1, rows) for piece in (low, high)]

    def order(j, half):
        if j == 0:
            if square:
                return [(0, 0), (0, 1), (1, 1), (2, 0)] if half == 0 else [(1, 0), (2, 1), (3, 0), (3, 1)]
            span = range(rows // 2) if half == 0 else range(rows // 2, rows)
            return [(d, t) for d in span for t in range(tiles)]
        return [(d, half) for d in range(rows)]

    def word_copy(j):
        return send(
            words_out.at[j - 1],
            words.at[j],
            word_send.at[j],
            word_recv.at[j],
            (r, reader(j) * 2 + k),
        )

    query_copy(1).start()
    for j in range(1, planes):
        for tile in range(tiles):
            line_copy(j, tile).start()
    for copy in spread_copies(0, 0):
        copy.start()
    query_copy(0).start()

    k_tiles = rows * tiles
    entries = 2 * 2 * tiles * k_tiles

    def gather_words(j, dst):
        first = reader(j) // 2 * entries

        def step(s, carry):
            for u in range(8):
                e = s * 8 + u
                entry = table_ref[first + e]
                dst[e] = masks_ref[jnp.maximum(entry, 0)] * jnp.where(entry >= 0, 1, 0)
            return carry

        lax.fori_loop(0, entries // 8, step, 0)

    for copy in loads:
        copy.wait()
    for j in range(1, planes):
        gather_words(j, words_out.at[j - 1])
        word_copy(j).start()

    kf[0, r] = features_ref[...]
    qf[0] = features_ref[...]
    wq_t[...] = wq_ref[...].T
    wv_t[...] = wv_ref[...].T
    half_keys = rows * nodes // 2
    for n in range(2 * planes):
        v_all[n, :, head : head + ONES, :] = jnp.ones((HEADS, ONES, half_keys), jnp.bfloat16)
    gather_words(0, words.at[0])

    def project(j, half, spot):
        block = jnp.concatenate(
            [
                kf[j, row_from(d), t * TILE : (t + 1) * TILE, :]
                for d, t in order(j, half)[spot : spot + 2]
            ],
            axis=0,
        )
        n = 2 * j + half
        lane = slice(spot * TILE, (spot + 2) * TILE)
        key = jnp.dot(block, wk_ref[...], preferred_element_type=f32)
        left = lax.broadcasted_iota(jnp.int32, (2 * TILE, 2 * head), 1) < head
        for p in range(HEADS // 2):
            both = key[:, p * 2 * head : (p + 1) * 2 * head]
            turned = pltpu.roll(both, head, 1)
            k_all[n, 2 * p, lane, :] = jnp.where(left, both, turned).astype(jnp.bfloat16)
            k_all[n, 2 * p + 1, lane, :] = jnp.where(left, turned, both).astype(jnp.bfloat16)
        value = lax.dot_general(
            wv_t[...], block, (((1,), (1,)), ((), ())), preferred_element_type=f32
        ).astype(jnp.bfloat16)
        for h in range(HEADS):
            v_all[n, h, :head, lane] = value[h * head : (h + 1) * head, :]

    def begin(j, half):
        for d, piece in late_pieces(j, half):
            await_piece(j, d, piece)
        for spot in range(2 if (j, half) == (0, 0) else 0, rows * tiles // 2, 2):
            project(j, half, spot)
        if j > 0 and half == 0:
            word_copy(j).wait_recv()

    def pair_copies(i, n, which):
        return (
            send(
                part.at[i, 1],
                mate_part.at[n, which],
                pair_send.at[n, which, 0],
                pair_recv.at[n, which, 0],
                mate,
            ),
            send(
                stat.at[i, 1],
                mate_stat.at[n, which],
                pair_send.at[n, which, 1],
                pair_recv.at[n, which, 1],
                mate,
            ),
        )

    fin_copies = (
        send(both_part, fin_part, fin_send.at[0], fin_recv.at[0], partner),
        send(both_stat, fin_stat, fin_send.at[1], fin_recv.at[1], partner),
    )

    def weigh(sources):
        peaks = [ref[0:HEADS, :] for _, ref in sources]
        top = functools.reduce(jnp.maximum, peaks)
        weights = [
            jnp.exp2(peak - top) * ref[HEADS : 2 * HEADS, :]
            for peak, (_, ref) in zip(peaks, sources)
        ]
        total = functools.reduce(jnp.add, weights)
        return top, weights, total

    def mixed(sources, weights, h):
        rows_of = slice(h * head, (h + 1) * head)
        return functools.reduce(
            jnp.add,
            [
                ref[rows_of, :].astype(f32) * weight[h : h + 1, :]
                for weight, (ref, _) in zip(weights, sources)
            ],
        )

    def turn_of(j, half, which):
        if j < last:
            return j * STEPS + half * 2 + which
        return j * STEPS + FINAL.index((half, which))

    def gathered(which):
        sources = []
        for j in range(planes):
            for half in range(2):
                n = 2 * j + half
                for copy in pair_copies(0, n, which):
                    copy.wait_recv()
                i = turn_of(j, half, which)
                sources.append((part.at[i, 0], stat.at[i, 0]))
                sources.append((mate_part.at[n, which], mate_stat.at[n, which]))
        return sources

    project(0, 0, 0)
    relay(0, 0)

    factor = math.log2(math.e) / math.sqrt(head)

    def queries(which, s):
        value = lax.dot_general(
            wq_t[...], qf[2 * which + s], (((1,), (1,)), ((), ())), preferred_element_type=f32
        )
        value = value.astype(jnp.bfloat16).astype(f32) * factor
        high = value.astype(jnp.bfloat16)
        low = (value - high.astype(f32)).astype(jnp.bfloat16)
        for h in range(HEADS):
            rows_of = slice(h * head, (h + 1) * head)
            q_all[which, s, h, :head, :] = high[rows_of, :]
            q_all[which, s, h, head:, :] = low[rows_of, :]

    def await_query(slot):
        send(qf.at[slot], qf.at[slot], q_send.at[0], q_recv.at[slot], mate).wait_recv()

    def turn(i, carry):
        j = i // STEPS
        u = lax.rem(i, STEPS)
        ending = j == last
        half = jnp.where(ending, pick([a for a, _ in FINAL], u), u // 2)
        which = jnp.where(ending, pick([b for _, b in FINAL], u), lax.rem(u, 2))
        n = 2 * j + half
        chip = jnp.where(which == 0, m, other)

        @pl.when(i == turn_of(0, 0, 1))
        def _():
            query_copy(1).wait_recv()
            query_copy(2).start()

        for plane in range(1, planes):
            base = (plane - 1) * STEPS
            for unit in range(tiles):

                @pl.when(i == base + unit + 2)
                def _():
                    line_copy(plane, unit).wait_recv()
                    for copy in spread_copies(plane, unit):
                        copy.start()

                @pl.when(i == base + unit + 3)
                def _():
                    relay(plane, unit)

        for plane in range(planes):
            for part_of in range(2):

                @pl.when(i == min(turn_of(plane, part_of, 0), turn_of(plane, part_of, 1)))
                def _():
                    begin(plane, part_of)

        for pair in range(2):

            @pl.when(i == turn_of(0, 0, pair))
            def _():
                queries(pair, 0)
                await_query(2 * pair + 1)
                queries(pair, 1)

        @pl.when(i == last * STEPS + 2)
        def _():
            sources = gathered(1)
            top, weights, total = weigh(sources)
            both_stat[0:HEADS, :] = top
            both_stat[HEADS : 2 * HEADS, :] = total
            for h in range(HEADS):
                both_part[h * head : (h + 1) * head, :] = (
                    mixed(sources, weights, h) / total[h : h + 1, :]
                ).astype(jnp.bfloat16)
            for copy in fin_copies:
                copy.start()

        spots = []
        for spot in range(rows * tiles // 2):
            choices = [order(0, 0)[spot], order(0, 1)[spot], order(1, 0)[spot], order(1, 1)[spot]]
            index = [row_from(d) * tiles + t for d, t in choices]
            spots.append(
                jnp.where(
                    j == 0,
                    jnp.where(half == 0, index[0], index[1]),
                    jnp.where(half == 0, index[2], index[3]),
                )
            )
        for s in range(2):
            lane = k if s == 0 else 1 - k
            first = (lax.rem(chip, 2) * 2 + lane) * tiles * k_tiles
            build_bias(words.at[j], first, k_tiles, spots, bias.at[s])

        attend(q_all.at[which], k_all.at[n], v_all.at[n], part.at[i], stat.at[i], bias, score)

        for copy in pair_copies(i, n, which):
            copy.start()

        return carry

    lax.fori_loop(0, turns, turn, 0)

    sources = gathered(0)
    top, weights, total = weigh(sources)
    for h in range(HEADS):
        numer[h * head : (h + 1) * head, :] = mixed(sources, weights, h)
    for copy in fin_copies:
        copy.wait_recv()
    peak = jnp.maximum(top, fin_stat[0:HEADS, :])
    mine = jnp.exp2(top - peak)
    theirs = jnp.exp2(fin_stat[0:HEADS, :] - peak) * fin_stat[HEADS : 2 * HEADS, :]
    den = total * mine + theirs
    mine, theirs = mine / den, theirs / den
    for h in range(HEADS):
        rows_of = slice(h * head, (h + 1) * head)
        attended[rows_of, :] = (
            numer[rows_of, :] * mine[h : h + 1, :]
            + fin_part[rows_of, :].astype(f32) * theirs[h : h + 1, :]
        ).astype(jnp.bfloat16)
    out_ref[...] = lax.dot_general(
        attended[...], wo_ref[...], (((0,), (0,)), ((), ())), preferred_element_type=f32
    ).astype(jnp.bfloat16)

    for step in range(3):
        query_copy(step).wait_send()
    for j in range(planes):
        for unit in range(tiles if j else 1):
            for copy in spread_copies(j, unit) + relay_copies(j, unit):
                copy.wait_send()
        if j:
            for tile in range(tiles):
                line_copy(j, tile).wait_send()
            word_copy(j).wait_send()
    for n in range(2 * planes):
        for which in range(2):
            for copy in pair_copies(0, n, which):
                copy.wait_send()
    for copy in fin_copies:
        copy.wait_send()


def fused(mesh_shape, table, masks, features, w_query, w_key, w_value, w_out):
    rows, cols = mesh_shape["row"], mesh_shape["col"]
    planes = cols // 4
    turns = planes * STEPS
    nodes, width = features.shape
    keys = rows * nodes // 2
    head = width // HEADS
    tiles = nodes // TILE
    entries = 2 * 2 * tiles * rows * tiles
    bf16, f32, i32 = jnp.bfloat16, jnp.float32, jnp.int32
    whole = pl.BlockSpec(memory_space=pltpu.VMEM)
    hbm = pl.BlockSpec(memory_space=pl.ANY)
    dma = pltpu.SemaphoreType.DMA
    return pl.pallas_call(
        functools.partial(fused_kernel, rows, cols),
        out_shape=jax.ShapeDtypeStruct((nodes, w_out.shape[1]), bf16),
        in_specs=[pl.BlockSpec(memory_space=pltpu.SMEM), hbm, whole] + [hbm] * 4,
        out_specs=whole,
        scratch_shapes=[
            pltpu.VMEM(masks.shape, i32),
            pltpu.VMEM((width, width), bf16),
            pltpu.VMEM((width, width), bf16),
            pltpu.VMEM((width, width), bf16),
            pltpu.VMEM(w_out.shape, bf16),
            pltpu.VMEM((planes, rows, nodes, width), bf16),
            pltpu.VMEM((4, nodes, width), bf16),
            pltpu.VMEM((width, width), bf16),
            pltpu.VMEM((width, width), bf16),
            pltpu.VMEM((max(planes - 1, 1), entries, TILE // 32, TILE), i32),
            pltpu.VMEM((planes, entries, TILE // 32, TILE), i32),
            pltpu.VMEM((2 * planes, HEADS, keys, 2 * head), bf16),
            pltpu.VMEM((2 * planes, HEADS, head + ONES, keys), bf16),
            pltpu.VMEM((2, 2, HEADS, 2 * head, nodes), bf16),
            pltpu.VMEM((turns, 2, width, nodes), bf16),
            pltpu.VMEM((turns, 2, 2 * HEADS, nodes), f32),
            pltpu.VMEM((2 * planes, 2, width, nodes), bf16),
            pltpu.VMEM((2 * planes, 2, 2 * HEADS, nodes), f32),
            pltpu.VMEM((width, nodes), bf16),
            pltpu.VMEM((2 * HEADS, nodes), f32),
            pltpu.VMEM((width, nodes), bf16),
            pltpu.VMEM((2 * HEADS, nodes), f32),
            pltpu.VMEM((width, nodes), f32),
            pltpu.VMEM((width, nodes), bf16),
            pltpu.VMEM((2, keys, nodes), f32),
            pltpu.VMEM((2, 2, keys, nodes), f32),
            dma((3,)),
            dma((4,)),
            dma((planes, tiles)),
            dma((planes, tiles)),
            dma((planes, rows, rows, 2 * tiles)),
            dma((planes, rows, 2 * tiles)),
            dma((planes,)),
            dma((planes,)),
            dma((2 * planes, 2, 2)),
            dma((2 * planes, 2, 2)),
            dma((2,)),
            dma((2,)),
            dma((5,)),
        ],
        compiler_params=pltpu.CompilerParams(
            collective_id=0, has_side_effects=True, vmem_limit_bytes=63 * 1024 * 1024
        ),
        name="fused",
    )(table, masks, features, w_query, w_key, w_value, w_out)


def entry_table(pairs, count, q_tiles, k_tiles):
    entries = pairs.shape[0]
    ids = lax.broadcasted_iota(jnp.int32, (q_tiles * k_tiles, entries), 1)
    cell = lax.broadcasted_iota(jnp.int32, (q_tiles * k_tiles, entries), 0)
    code = (pairs[:, 0] * k_tiles + pairs[:, 1])[None, :]
    return jnp.max(jnp.where((code == cell) & (ids < count), ids, -1), axis=1)


def body(mesh_shape, features, w_query, w_key, w_value, w_out, pairs, counts, masks):
    nodes = features.shape[0]
    rows, cols = mesh_shape["row"], mesh_shape["col"]
    table = entry_table(pairs[0, 0], counts[0, 0], cols * nodes // TILE, rows * nodes // TILE)
    words = masks[0, 0].transpose(0, 2, 1)
    return fused(mesh_shape, table, words, features, w_query, w_key, w_value, w_out)


def solution(mesh):
    in_specs = (
        P(("row", "col"), None),
        P(),
        P(),
        P(),
        P(),
        P("row", "col", None, None),
        P("row", "col"),
        P("row", "col", None, None, None),
    )
    out_specs = P(("row", "col"), None)
    return jax.shard_map(
        functools.partial(body, dict(mesh.shape)), mesh=mesh, in_specs=in_specs, out_specs=out_specs, check_vma=False)
```

```python
import functools
import math

import jax
import jax.numpy as jnp
from jax import lax
from jax.experimental import pallas as pl
from jax.experimental.pallas import tpu as pltpu
from jax.sharding import PartitionSpec as P

HEADS = 8
TILE = 128
BLOCK = 256
ONES = 16
MESH = pl.DeviceIdType.MESH
STEPS = 4
SPREAD = (1, 3)
FINAL = ((0, 1), (1, 1), (0, 0), (1, 0))


def build_bias(words_ref, first, k_tiles, spots, bias_ref):
    span = bias_ref.shape[1]
    tiles = span // TILE
    shift = 31 - lax.broadcasted_iota(jnp.int32, (32, TILE), 0)
    for b, spot in enumerate(spots):
        for t in range(tiles):
            words = words_ref[first + t * k_tiles + spot]
            for j in range(TILE // 32):
                bits = jnp.broadcast_to(words[j : j + 1, :], (32, TILE)) << shift
                bias_ref[pl.ds(b * TILE + j * 32, 32), pl.ds(t * TILE, TILE)] = jnp.where(
                    bits < 0, 0.0, -jnp.inf
                )


def attend(q_ref, k_ref, v_ref, part_ref, stat_ref, bias_ref, score_ref, middle):
    heads, keys, _ = k_ref.shape
    span = q_ref.shape[3]
    head = v_ref.shape[1] - ONES
    blocks = keys // BLOCK
    zero = jnp.zeros((8, span), jnp.float32)

    def scores(h, s, block, top):
        rows = slice(block * BLOCK, (block + 1) * BLOCK)
        raw = jnp.dot(k_ref[h, rows, :], q_ref[s, h], preferred_element_type=jnp.float32)
        raw = raw + bias_ref[s, rows, :]
        score_ref[h % 2, s, rows, :] = raw
        return jnp.maximum(top, jnp.max(raw.reshape(BLOCK // 8, 8, span), axis=0))

    def weighted(h, s, block, top, total):
        rows = slice(block * BLOCK, (block + 1) * BLOCK)
        prob = jnp.exp2(score_ref[h % 2, s, rows, :] - top).astype(jnp.bfloat16)
        term = jnp.dot(v_ref[h, :, rows], prob, preferred_element_type=jnp.float32)
        return term if total is None else total + term

    def finish(h, s, top, total):
        den = total[head : head + 1, :] + jnp.exp2(-top)
        part_ref[s, h * head : (h + 1) * head, :] = (total[:head, :] / den).astype(jnp.bfloat16)
        stat_ref[s, h : h + 1, :] = top
        stat_ref[s, heads + h : heads + h + 1, :] = den

    tops = [zero, zero]
    for s in range(2):
        for block in range(blocks):
            tops[s] = scores(0, s, block, tops[s])
    for h in range(heads):
        if h == heads // 2:
            middle()
        later = [zero, zero]
        for s in range(2):
            top = jnp.max(tops[s], axis=0, keepdims=True)
            total = None
            for block in range(blocks):
                if h + 1 < heads:
                    later[s] = scores(h + 1, s, block, later[s])
                total = weighted(h, s, block, top, total)
            finish(h, s, top, total)
        tops = later


def pick(values, index):
    out = values[0]
    for n, value in enumerate(values[1:]):
        out = jnp.where(index == n + 1, value, out)
    return out


def fused_kernel(
    rows,
    cols,
    table_ref,
    masks_hbm,
    features_ref,
    wq_hbm,
    wk_hbm,
    wv_hbm,
    wo_hbm,
    out_ref,
    masks_ref,
    wq_ref,
    wk_ref,
    wv_ref,
    wo_ref,
    kf,
    qf,
    wq_t,
    wv_t,
    words_out,
    words,
    k_all,
    v_all,
    q_all,
    part,
    stat,
    mate_part,
    mate_stat,
    both_part,
    both_stat,
    fin_part,
    fin_stat,
    numer,
    attended,
    bias,
    score,
    q_send,
    q_recv,
    z_send,
    z_recv,
    row_send,
    row_recv,
    word_send,
    word_recv,
    pair_send,
    pair_recv,
    fin_send,
    fin_recv,
    load,
):
    nodes, width = features_ref.shape
    head = width // HEADS
    f32 = jnp.float32
    chips = cols // 2
    planes = chips // 2
    last = planes - 1
    turns = planes * STEPS
    tiles = nodes // TILE
    square = rows == 4
    r, c = lax.axis_index("row"), lax.axis_index("col")
    m, k = c // 2, lax.rem(c, 2)
    other = m + 1 - 2 * lax.rem(m, 2)
    mate = (r, m * 2 + 1 - k)
    partner = (r, other * 2 + k)

    def reader(j):
        return lax.rem(m + chips - 2 * j, chips)

    def flip(place, b):
        return place + 1 - 2 * lax.rem(place, 2) if b else place

    def row_to(d):
        if rows % 2:
            return lax.rem(r + d, rows)
        return flip(lax.rem(r + d // 2 * 2, rows), d % 2)

    def row_from(d):
        if rows % 2:
            return lax.rem(r + rows - d, rows)
        return lax.rem(flip(r, d % 2) + rows - d // 2 * 2, rows)

    def send(src, dst, send_sem, recv_sem, device):
        return pltpu.make_async_remote_copy(
            src_ref=src,
            dst_ref=dst,
            send_sem=send_sem,
            recv_sem=recv_sem,
            device_id=device,
            device_id_type=MESH,
        )

    loads = [
        pltpu.make_async_copy(src, dst, load.at[n])
        for n, (src, dst) in enumerate(
            (
                (masks_hbm, masks_ref),
                (wk_hbm, wk_ref),
                (wv_hbm, wv_ref),
                (wq_hbm, wq_ref),
                (wo_hbm, wo_ref),
            )
        )
    ]
    barrier = pltpu.get_barrier_semaphore()
    peers = [mate, partner]
    peers += [(lax.rem(r + d, rows), c) for d in range(1, rows)]
    peers += [(r, reader(j) * 2 + k) for j in range(1, planes)]
    for peer in peers:
        pl.semaphore_signal(barrier, inc=1, device_id=peer, device_id_type=MESH)
    for copy in loads:
        copy.start()
    pl.semaphore_wait(barrier, len(peers))

    def query_copy(step):
        if step == 0:
            return send(features_ref, qf.at[1], q_send.at[0], q_recv.at[1], mate)
        if step == 1:
            return send(features_ref, qf.at[2], q_send.at[1], q_recv.at[2], partner)
        return send(qf.at[2], qf.at[3], q_send.at[2], q_recv.at[3], mate)

    def line_copy(j, tile):
        span = pl.ds(tile * TILE, TILE)
        return send(
            features_ref.at[span],
            kf.at[j, r, span],
            z_send.at[j, tile],
            z_recv.at[j, tile],
            (r, reader(j) * 2 + k),
        )

    def pieces(j, unit):
        if j == 0:
            return (0, TILE, 0), (TILE, TILE, 1)
        return ((unit * TILE, TILE, unit),)

    def row_copy(j, row, d, piece, own=False):
        start, size, n = piece
        span = pl.ds(start, size)
        return send(
            features_ref.at[span] if own else kf.at[j, row, span],
            kf.at[j, row, span],
            row_send.at[j, row, d, n],
            row_recv.at[j, row, n],
            (row_to(d), c),
        )

    def spread_copies(j, unit):
        own = j == 0
        if own and square:
            low, high = pieces(0, 0)
            order = [(1, high), (2, low), (1, low), (2, high)]
        else:
            order = [(d, piece) for piece in pieces(j, unit) for d in reversed(range(1, rows))]
        return [row_copy(j, r, d, piece, own) for d, piece in order]

    def relay_copies():
        if not square:
            return []
        low, high = pieces(0, 0)
        return [row_copy(0, row_from(1), 2, high), row_copy(0, row_from(2), 1, low)]

    def await_piece(j, d, piece):
        row_copy(j, row_from(d), 1, piece).wait_recv()

    def relay():
        low, high = pieces(0, 0)
        for copy, d, piece in zip(relay_copies(), (1, 2), (high, low)):
            await_piece(0, d, piece)
            copy.start()

    def late_pieces(j, half):
        if j == 0:
            low, high = pieces(0, 0)
            if square:
                return [] if half == 0 else [(1, low), (2, high), (3, low), (3, high)]
            span = range(1, rows // 2) if half == 0 else range(rows // 2, rows)
            return [(d, piece) for d in span for piece in (low, high)]
        return [(d, piece) for d in range(1, rows) for piece in pieces(j, half)]

    def order(j, half):
        if j == 0:
            if square:
                return [(0, 0), (0, 1), (1, 1), (2, 0)] if half == 0 else [(1, 0), (2, 1), (3, 0), (3, 1)]
            span = range(rows // 2) if half == 0 else range(rows // 2, rows)
            return [(d, t) for d in span for t in range(tiles)]
        return [(d, half) for d in range(rows)]

    def word_copy(j):
        return send(
            words_out.at[j - 1],
            words.at[j],
            word_send.at[j],
            word_recv.at[j],
            (r, reader(j) * 2 + k),
        )

    query_copy(1).start()
    for j in range(1, planes):
        for tile in range(tiles):
            line_copy(j, tile).start()
    for copy in spread_copies(0, 0):
        copy.start()
    query_copy(0).start()

    k_tiles = rows * tiles
    entries = 2 * 2 * tiles * k_tiles

    def gather_words(j, dst):
        first = reader(j) // 2 * entries

        def step(s, carry):
            for u in range(8):
                e = s * 8 + u
                entry = table_ref[first + e]
                dst[e] = masks_ref[jnp.maximum(entry, 0)] * jnp.where(entry >= 0, 1, 0)
            return carry

        lax.fori_loop(0, entries // 8, step, 0)

    for copy in loads:
        copy.wait()
    for j in range(1, planes):
        gather_words(j, words_out.at[j - 1])
        word_copy(j).start()

    kf[0, r] = features_ref[...]
    qf[0] = features_ref[...]
    wq_t[...] = wq_ref[...].T
    wv_t[...] = wv_ref[...].T
    half_keys = rows * nodes // 2
    for n in range(2 * planes):
        v_all[n, :, head : head + ONES, :] = jnp.ones((HEADS, ONES, half_keys), jnp.bfloat16)
    gather_words(0, words.at[0])

    def project(j, half, spot):
        block = jnp.concatenate(
            [
                kf[j, row_from(d), t * TILE : (t + 1) * TILE, :]
                for d, t in order(j, half)[spot : spot + 2]
            ],
            axis=0,
        )
        n = 2 * j + half
        lane = slice(spot * TILE, (spot + 2) * TILE)
        key = jnp.dot(block, wk_ref[...], preferred_element_type=f32)
        left = lax.broadcasted_iota(jnp.int32, (2 * TILE, 2 * head), 1) < head
        for p in range(HEADS // 2):
            both = key[:, p * 2 * head : (p + 1) * 2 * head]
            turned = pltpu.roll(both, head, 1)
            k_all[n, 2 * p, lane, :] = jnp.where(left, both, turned).astype(jnp.bfloat16)
            k_all[n, 2 * p + 1, lane, :] = jnp.where(left, turned, both).astype(jnp.bfloat16)
        value = lax.dot_general(
            wv_t[...], block, (((1,), (1,)), ((), ())), preferred_element_type=f32
        ).astype(jnp.bfloat16)
        for h in range(HEADS):
            v_all[n, h, :head, lane] = value[h * head : (h + 1) * head, :]

    def begin(j, half):
        for d, piece in late_pieces(j, half):
            await_piece(j, d, piece)
        for spot in range(2 if (j, half) == (0, 0) else 0, rows * tiles // 2, 2):
            project(j, half, spot)
        if j > 0 and half == 0:
            word_copy(j).wait_recv()

    def pair_copies(i, n, which):
        return (
            send(
                part.at[i, 1],
                mate_part.at[n, which],
                pair_send.at[n, which, 0],
                pair_recv.at[n, which, 0],
                mate,
            ),
            send(
                stat.at[i, 1],
                mate_stat.at[n, which],
                pair_send.at[n, which, 1],
                pair_recv.at[n, which, 1],
                mate,
            ),
        )

    fin_copies = (
        send(both_part, fin_part, fin_send.at[0], fin_recv.at[0], partner),
        send(both_stat, fin_stat, fin_send.at[1], fin_recv.at[1], partner),
    )

    def weigh(sources):
        peaks = [ref[0:HEADS, :] for _, ref in sources]
        top = functools.reduce(jnp.maximum, peaks)
        weights = [
            jnp.exp2(peak - top) * ref[HEADS : 2 * HEADS, :]
            for peak, (_, ref) in zip(peaks, sources)
        ]
        total = functools.reduce(jnp.add, weights)
        return top, weights, total

    def mixed(sources, weights, h):
        rows_of = slice(h * head, (h + 1) * head)
        return functools.reduce(
            jnp.add,
            [
                ref[rows_of, :].astype(f32) * weight[h : h + 1, :]
                for weight, (ref, _) in zip(weights, sources)
            ],
        )

    def turn_of(j, half, which):
        if j < last:
            return j * STEPS + half * 2 + which
        return j * STEPS + FINAL.index((half, which))

    def gathered(which):
        sources = []
        for j in range(planes):
            for half in range(2):
                n = 2 * j + half
                for copy in pair_copies(0, n, which):
                    copy.wait_recv()
                i = turn_of(j, half, which)
                sources.append((part.at[i, 0], stat.at[i, 0]))
                sources.append((mate_part.at[n, which], mate_stat.at[n, which]))
        return sources

    project(0, 0, 0)
    relay()

    factor = math.log2(math.e) / math.sqrt(head)

    def queries(which, s):
        value = lax.dot_general(
            wq_t[...], qf[2 * which + s], (((1,), (1,)), ((), ())), preferred_element_type=f32
        )
        value = value.astype(jnp.bfloat16).astype(f32) * factor
        high = value.astype(jnp.bfloat16)
        low = (value - high.astype(f32)).astype(jnp.bfloat16)
        for h in range(HEADS):
            rows_of = slice(h * head, (h + 1) * head)
            q_all[which, s, h, :head, :] = high[rows_of, :]
            q_all[which, s, h, head:, :] = low[rows_of, :]

    def await_query(slot):
        send(qf.at[slot], qf.at[slot], q_send.at[0], q_recv.at[slot], mate).wait_recv()

    def turn(i, carry):
        j = i // STEPS
        u = lax.rem(i, STEPS)
        ending = j == last
        half = jnp.where(ending, pick([a for a, _ in FINAL], u), u // 2)
        which = jnp.where(ending, pick([b for _, b in FINAL], u), lax.rem(u, 2))
        n = 2 * j + half
        chip = jnp.where(which == 0, m, other)

        @pl.when(i == turn_of(0, 0, 1))
        def _():
            query_copy(1).wait_recv()
            query_copy(2).start()

        def forward(late):
            for plane in range(1, planes):
                base = (plane - 1) * STEPS
                for unit in range(tiles):
                    if SPREAD[unit] % 2 == late:

                        @pl.when(i == base + SPREAD[unit] // 2)
                        def _():
                            line_copy(plane, unit).wait_recv()
                            for copy in spread_copies(plane, unit):
                                copy.start()

        forward(0)

        for plane in range(planes):
            for part_of in range(2):

                @pl.when(i == min(turn_of(plane, part_of, 0), turn_of(plane, part_of, 1)))
                def _():
                    begin(plane, part_of)

        for pair in range(2):

            @pl.when(i == turn_of(0, 0, pair))
            def _():
                queries(pair, 0)
                await_query(2 * pair + 1)
                queries(pair, 1)

        @pl.when(i == last * STEPS + 2)
        def _():
            sources = gathered(1)
            top, weights, total = weigh(sources)
            both_stat[0:HEADS, :] = top
            both_stat[HEADS : 2 * HEADS, :] = total
            for h in range(HEADS):
                both_part[h * head : (h + 1) * head, :] = (
                    mixed(sources, weights, h) / total[h : h + 1, :]
                ).astype(jnp.bfloat16)
            for copy in fin_copies:
                copy.start()

        spots = []
        for spot in range(rows * tiles // 2):
            choices = [order(0, 0)[spot], order(0, 1)[spot], order(1, 0)[spot], order(1, 1)[spot]]
            index = [row_from(d) * tiles + t for d, t in choices]
            spots.append(
                jnp.where(
                    j == 0,
                    jnp.where(half == 0, index[0], index[1]),
                    jnp.where(half == 0, index[2], index[3]),
                )
            )
        for s in range(2):
            lane = k if s == 0 else 1 - k
            first = (lax.rem(chip, 2) * 2 + lane) * tiles * k_tiles
            build_bias(words.at[j], first, k_tiles, spots, bias.at[s])

        attend(q_all.at[which], k_all.at[n], v_all.at[n], part.at[i], stat.at[i], bias, score,
            lambda: forward(1))

        for copy in pair_copies(i, n, which):
            copy.start()

        return carry

    lax.fori_loop(0, turns, turn, 0)

    sources = gathered(0)
    top, weights, total = weigh(sources)
    for h in range(HEADS):
        numer[h * head : (h + 1) * head, :] = mixed(sources, weights, h)
    for copy in fin_copies:
        copy.wait_recv()
    peak = jnp.maximum(top, fin_stat[0:HEADS, :])
    mine = jnp.exp2(top - peak)
    theirs = jnp.exp2(fin_stat[0:HEADS, :] - peak) * fin_stat[HEADS : 2 * HEADS, :]
    den = total * mine + theirs
    mine, theirs = mine / den, theirs / den
    for h in range(HEADS):
        rows_of = slice(h * head, (h + 1) * head)
        attended[rows_of, :] = (
            numer[rows_of, :] * mine[h : h + 1, :]
            + fin_part[rows_of, :].astype(f32) * theirs[h : h + 1, :]
        ).astype(jnp.bfloat16)
    out_ref[...] = lax.dot_general(
        attended[...], wo_ref[...], (((0,), (0,)), ((), ())), preferred_element_type=f32
    ).astype(jnp.bfloat16)

    for step in range(3):
        query_copy(step).wait_send()
    for j in range(planes):
        for unit in range(tiles if j else 1):
            for copy in spread_copies(j, unit) + ([] if j else relay_copies()):
                copy.wait_send()
        if j:
            for tile in range(tiles):
                line_copy(j, tile).wait_send()
            word_copy(j).wait_send()
    for n in range(2 * planes):
        for which in range(2):
            for copy in pair_copies(0, n, which):
                copy.wait_send()
    for copy in fin_copies:
        copy.wait_send()


def fused(mesh_shape, table, masks, features, w_query, w_key, w_value, w_out):
    rows, cols = mesh_shape["row"], mesh_shape["col"]
    planes = cols // 4
    turns = planes * STEPS
    nodes, width = features.shape
    keys = rows * nodes // 2
    head = width // HEADS
    tiles = nodes // TILE
    entries = 2 * 2 * tiles * rows * tiles
    bf16, f32, i32 = jnp.bfloat16, jnp.float32, jnp.int32
    whole = pl.BlockSpec(memory_space=pltpu.VMEM)
    hbm = pl.BlockSpec(memory_space=pl.ANY)
    dma = pltpu.SemaphoreType.DMA
    return pl.pallas_call(
        functools.partial(fused_kernel, rows, cols),
        out_shape=jax.ShapeDtypeStruct((nodes, w_out.shape[1]), bf16),
        in_specs=[pl.BlockSpec(memory_space=pltpu.SMEM), hbm, whole] + [hbm] * 4,
        out_specs=whole,
        scratch_shapes=[
            pltpu.VMEM(masks.shape, i32),
            pltpu.VMEM((width, width), bf16),
            pltpu.VMEM((width, width), bf16),
            pltpu.VMEM((width, width), bf16),
            pltpu.VMEM(w_out.shape, bf16),
            pltpu.VMEM((planes, rows, nodes, width), bf16),
            pltpu.VMEM((4, nodes, width), bf16),
            pltpu.VMEM((width, width), bf16),
            pltpu.VMEM((width, width), bf16),
            pltpu.VMEM((max(planes - 1, 1), entries, TILE // 32, TILE), i32),
            pltpu.VMEM((planes, entries, TILE // 32, TILE), i32),
            pltpu.VMEM((2 * planes, HEADS, keys, 2 * head), bf16),
            pltpu.VMEM((2 * planes, HEADS, head + ONES, keys), bf16),
            pltpu.VMEM((2, 2, HEADS, 2 * head, nodes), bf16),
            pltpu.VMEM((turns, 2, width, nodes), bf16),
            pltpu.VMEM((turns, 2, 2 * HEADS, nodes), f32),
            pltpu.VMEM((2 * planes, 2, width, nodes), bf16),
            pltpu.VMEM((2 * planes, 2, 2 * HEADS, nodes), f32),
            pltpu.VMEM((width, nodes), bf16),
            pltpu.VMEM((2 * HEADS, nodes), f32),
            pltpu.VMEM((width, nodes), bf16),
            pltpu.VMEM((2 * HEADS, nodes), f32),
            pltpu.VMEM((width, nodes), f32),
            pltpu.VMEM((width, nodes), bf16),
            pltpu.VMEM((2, keys, nodes), f32),
            pltpu.VMEM((2, 2, keys, nodes), f32),
            dma((3,)),
            dma((4,)),
            dma((planes, tiles)),
            dma((planes, tiles)),
            dma((planes, rows, rows, 2 * tiles)),
            dma((planes, rows, 2 * tiles)),
            dma((planes,)),
            dma((planes,)),
            dma((2 * planes, 2, 2)),
            dma((2 * planes, 2, 2)),
            dma((2,)),
            dma((2,)),
            dma((5,)),
        ],
        compiler_params=pltpu.CompilerParams(
            collective_id=0, has_side_effects=True, vmem_limit_bytes=67_043_328
        ),
        name="fused",
    )(table, masks, features, w_query, w_key, w_value, w_out)


def entry_table(pairs, count, q_tiles, k_tiles):
    entries = pairs.shape[0]
    ids = lax.broadcasted_iota(jnp.int32, (q_tiles * k_tiles, entries), 1)
    cell = lax.broadcasted_iota(jnp.int32, (q_tiles * k_tiles, entries), 0)
    code = (pairs[:, 0] * k_tiles + pairs[:, 1])[None, :]
    return jnp.max(jnp.where((code == cell) & (ids < count), ids, -1), axis=1)


def body(mesh_shape, features, w_query, w_key, w_value, w_out, pairs, counts, masks):
    nodes = features.shape[0]
    rows, cols = mesh_shape["row"], mesh_shape["col"]
    table = entry_table(pairs[0, 0], counts[0, 0], cols * nodes // TILE, rows * nodes // TILE)
    words = masks[0, 0].transpose(0, 2, 1)
    return fused(mesh_shape, table, words, features, w_query, w_key, w_value, w_out)


def solution(mesh):
    in_specs = (
        P(("row", "col"), None),
        P(),
        P(),
        P(),
        P(),
        P("row", "col", None, None),
        P("row", "col"),
        P("row", "col", None, None, None),
    )
    out_specs = P(("row", "col"), None)
    return jax.shard_map(
        functools.partial(body, dict(mesh.shape)), mesh=mesh, in_specs=in_specs, out_specs=out_specs, check_vma=False)
```

```python
import functools
import math

import jax
import jax.numpy as jnp
from jax import lax
from jax.experimental import pallas as pl
from jax.experimental.pallas import tpu as pltpu
from jax.sharding import PartitionSpec as P

HEADS = 8
TILE = 128
BLOCK = 256
ONES = 16
MESH = pl.DeviceIdType.MESH
STEPS = 4
SPREAD = (1, 3)
FINAL = ((0, 1), (1, 1), (0, 0), (1, 0))


def build_bias(words_ref, first, k_tiles, spots, bias_ref):
    span = bias_ref.shape[1]
    tiles = span // TILE
    shift = 31 - lax.broadcasted_iota(jnp.int32, (32, TILE), 0)
    for b, spot in enumerate(spots):
        for t in range(tiles):
            cell = first + t * k_tiles + spot
            for j in range(TILE // 32):
                bits = jnp.broadcast_to(words_ref[j, pl.ds(cell, 1), :], (32, TILE)) << shift
                bias_ref[pl.ds(b * TILE + j * 32, 32), pl.ds(t * TILE, TILE)] = jnp.where(
                    bits < 0, 0.0, -jnp.inf
                )


def attend(q_ref, k_ref, v_ref, part_ref, stat_ref, bias_ref, score_ref, middle):
    heads, keys, _ = k_ref.shape
    span = q_ref.shape[3]
    head = v_ref.shape[1] - ONES
    blocks = keys // BLOCK
    zero = jnp.zeros((8, span), jnp.float32)

    def scores(h, s, block, top):
        rows = slice(block * BLOCK, (block + 1) * BLOCK)
        raw = jnp.dot(k_ref[h, rows, :], q_ref[s, h], preferred_element_type=jnp.float32)
        raw = raw + bias_ref[s, rows, :]
        score_ref[h % 2, s, rows, :] = raw
        return jnp.maximum(top, jnp.max(raw.reshape(BLOCK // 8, 8, span), axis=0))

    def weighted(h, s, block, top, total):
        rows = slice(block * BLOCK, (block + 1) * BLOCK)
        prob = jnp.exp2(score_ref[h % 2, s, rows, :] - top).astype(jnp.bfloat16)
        term = jnp.dot(v_ref[h, :, rows], prob, preferred_element_type=jnp.float32)
        return term if total is None else total + term

    def finish(h, s, top, total):
        den = total[head : head + 1, :] + jnp.exp2(-top)
        part_ref[s, h * head : (h + 1) * head, :] = (total[:head, :] / den).astype(jnp.bfloat16)
        stat_ref[s, h : h + 1, :] = top
        stat_ref[s, heads + h : heads + h + 1, :] = den

    tops = [zero, zero]
    for s in range(2):
        for block in range(blocks):
            tops[s] = scores(0, s, block, tops[s])
    for h in range(heads):
        if h == heads // 2:
            middle()
        later = [zero, zero]
        for s in range(2):
            top = jnp.max(tops[s], axis=0, keepdims=True)
            total = None
            for block in range(blocks):
                if h + 1 < heads:
                    later[s] = scores(h + 1, s, block, later[s])
                total = weighted(h, s, block, top, total)
            finish(h, s, top, total)
        tops = later


def pick(values, index):
    out = values[0]
    for n, value in enumerate(values[1:]):
        out = jnp.where(index == n + 1, value, out)
    return out


def fused_kernel(
    rows,
    cols,
    count_ref,
    pairs_ref,
    masks_hbm,
    features_ref,
    wq_hbm,
    wk_hbm,
    wv_hbm,
    wo_hbm,
    out_ref,
    masks_ref,
    wq_ref,
    wk_ref,
    wv_ref,
    wo_ref,
    kf,
    qf,
    wq_t,
    wv_t,
    dense,
    words,
    k_all,
    v_all,
    q_all,
    part,
    stat,
    mate_part,
    mate_stat,
    both_part,
    both_stat,
    fin_part,
    fin_stat,
    attended,
    bias,
    score,
    q_send,
    q_recv,
    z_send,
    z_recv,
    row_send,
    row_recv,
    word_send,
    word_recv,
    pair_send,
    pair_recv,
    fin_send,
    fin_recv,
    load,
):
    nodes, width = features_ref.shape
    head = width // HEADS
    f32 = jnp.float32
    chips = cols // 2
    planes = chips // 2
    last = planes - 1
    turns = planes * STEPS
    tiles = nodes // TILE
    square = rows == 4
    r, c = lax.axis_index("row"), lax.axis_index("col")
    m, k = c // 2, lax.rem(c, 2)
    other = m + 1 - 2 * lax.rem(m, 2)
    mate = (r, m * 2 + 1 - k)
    partner = (r, other * 2 + k)

    def reader(j):
        return lax.rem(m + chips - 2 * j, chips)

    def flip(place, b):
        return place + 1 - 2 * lax.rem(place, 2) if b else place

    def row_to(d):
        if rows % 2:
            return lax.rem(r + d, rows)
        return flip(lax.rem(r + d // 2 * 2, rows), d % 2)

    def row_from(d):
        if rows % 2:
            return lax.rem(r + rows - d, rows)
        return lax.rem(flip(r, d % 2) + rows - d // 2 * 2, rows)

    def send(src, dst, send_sem, recv_sem, device):
        return pltpu.make_async_remote_copy(
            src_ref=src,
            dst_ref=dst,
            send_sem=send_sem,
            recv_sem=recv_sem,
            device_id=device,
            device_id_type=MESH,
        )

    loads = [
        pltpu.make_async_copy(src, dst, load.at[n])
        for n, (src, dst) in enumerate(
            (
                (masks_hbm, masks_ref),
                (wk_hbm, wk_ref),
                (wv_hbm, wv_ref),
                (wq_hbm, wq_ref),
                (wo_hbm, wo_ref),
            )
        )
    ]
    barrier = pltpu.get_barrier_semaphore()
    peers = [mate, partner]
    peers += [(lax.rem(r + d, rows), c) for d in range(1, rows)]
    peers += [(r, reader(j) * 2 + k) for j in range(1, planes)]
    for peer in peers:
        pl.semaphore_signal(barrier, inc=1, device_id=peer, device_id_type=MESH)
    for copy in loads:
        copy.start()
    pl.semaphore_wait(barrier, len(peers))

    def query_copy(step):
        if step == 0:
            return send(features_ref, qf.at[1], q_send.at[0], q_recv.at[1], mate)
        if step == 1:
            return send(features_ref, qf.at[2], q_send.at[1], q_recv.at[2], partner)
        return send(qf.at[2], qf.at[3], q_send.at[2], q_recv.at[3], mate)

    def line_copy(j, tile):
        span = pl.ds(tile * TILE, TILE)
        return send(
            features_ref.at[span],
            kf.at[j, r, span],
            z_send.at[j, tile],
            z_recv.at[j, tile],
            (r, reader(j) * 2 + k),
        )

    def pieces(j, unit):
        if j == 0:
            return (0, TILE, 0), (TILE, TILE, 1)
        return ((unit * TILE, TILE, unit),)

    def row_copy(j, row, d, piece, own=False):
        start, size, n = piece
        span = pl.ds(start, size)
        return send(
            features_ref.at[span] if own else kf.at[j, row, span],
            kf.at[j, row, span],
            row_send.at[j, row, d, n],
            row_recv.at[j, row, n],
            (row_to(d), c),
        )

    def spread_copies(j, unit):
        own = j == 0
        if own and square:
            low, high = pieces(0, 0)
            order = [(1, high), (2, low), (1, low), (2, high)]
        else:
            order = [(d, piece) for piece in pieces(j, unit) for d in reversed(range(1, rows))]
        return [row_copy(j, r, d, piece, own) for d, piece in order]

    def relay_copies():
        if not square:
            return []
        low, high = pieces(0, 0)
        return [row_copy(0, row_from(1), 2, high), row_copy(0, row_from(2), 1, low)]

    def await_piece(j, d, piece):
        row_copy(j, row_from(d), 1, piece).wait_recv()

    def relay():
        low, high = pieces(0, 0)
        for copy, d, piece in zip(relay_copies(), (1, 2), (high, low)):
            await_piece(0, d, piece)
            copy.start()

    def late_pieces(j, half):
        if j == 0:
            low, high = pieces(0, 0)
            if square:
                return [] if half == 0 else [(1, low), (2, high), (3, low), (3, high)]
            span = range(1, rows // 2) if half == 0 else range(rows // 2, rows)
            return [(d, piece) for d in span for piece in (low, high)]
        return [(d, piece) for d in range(1, rows) for piece in pieces(j, half)]

    def order(j, half):
        if j == 0:
            if square:
                return [(0, 0), (0, 1), (1, 1), (2, 0)] if half == 0 else [(1, 0), (2, 1), (3, 0), (3, 1)]
            span = range(rows // 2) if half == 0 else range(rows // 2, rows)
            return [(d, t) for d in span for t in range(tiles)]
        return [(d, half) for d in range(rows)]

    def word_copy(j):
        return send(
            dense.at[:, own_words(j)],
            words.at[j],
            word_send.at[j],
            word_recv.at[j],
            (r, reader(j) * 2 + k),
        )

    query_copy(1).start()
    for j in range(1, planes):
        for tile in range(tiles):
            line_copy(j, tile).start()
    for copy in spread_copies(0, 0):
        copy.start()
    query_copy(0).start()

    k_tiles = rows * tiles
    entries = 2 * 2 * tiles * k_tiles

    def scatter_words():
        listed = masks_ref.shape[0] // (TILE // 32)
        cells = dense.shape[1]
        code = pairs_ref[0:1, :] * k_tiles + pairs_ref[1:2, :]
        valid = lax.broadcasted_iota(jnp.int32, (1, listed), 1) < count_ref[0, 0]
        code = jnp.broadcast_to(jnp.where(valid, code, -1), (cells, listed))
        place = jnp.where(
            code == lax.broadcasted_iota(jnp.int32, (cells, listed), 0), 1.0, 0.0
        ).astype(jnp.bfloat16)
        for w in range(TILE // 32):
            word = masks_ref[pl.ds(w, listed, stride=TILE // 32), :]
            merged = None
            for b in range(4):
                byte = ((word >> (8 * b)) & 255).astype(f32).astype(jnp.bfloat16)
                moved = jnp.dot(place, byte, preferred_element_type=f32).astype(jnp.int32) << (8 * b)
                merged = moved if merged is None else merged | moved
            dense[w] = merged

    def own_words(j):
        return pl.ds(pl.multiple_of(reader(j) // 2 * entries, entries), entries)

    for copy in loads:
        copy.wait()
    scatter_words()

    kf[0, r] = features_ref[...]
    qf[0] = features_ref[...]
    wq_t[...] = wq_ref[...].T
    wv_t[...] = wv_ref[...].T
    half_keys = rows * nodes // 2
    for n in range(2 * planes):
        v_all[n, :, head : head + ONES, :] = jnp.ones((HEADS, ONES, half_keys), jnp.bfloat16)
    words[0] = dense[:, own_words(0), :]

    def project(j, half, spot):
        block = jnp.concatenate(
            [
                kf[j, row_from(d), t * TILE : (t + 1) * TILE, :]
                for d, t in order(j, half)[spot : spot + 2]
            ],
            axis=0,
        )
        n = 2 * j + half
        lane = slice(spot * TILE, (spot + 2) * TILE)
        key = jnp.dot(block, wk_ref[...], preferred_element_type=f32)
        left = lax.broadcasted_iota(jnp.int32, (2 * TILE, 2 * head), 1) < head
        for p in range(HEADS // 2):
            both = key[:, p * 2 * head : (p + 1) * 2 * head]
            turned = pltpu.roll(both, head, 1)
            k_all[n, 2 * p, lane, :] = jnp.where(left, both, turned).astype(jnp.bfloat16)
            k_all[n, 2 * p + 1, lane, :] = jnp.where(left, turned, both).astype(jnp.bfloat16)
        value = lax.dot_general(
            wv_t[...], block, (((1,), (1,)), ((), ())), preferred_element_type=f32
        ).astype(jnp.bfloat16)
        for h in range(HEADS):
            v_all[n, h, :head, lane] = value[h * head : (h + 1) * head, :]

    def begin(j, half):
        for d, piece in late_pieces(j, half):
            await_piece(j, d, piece)
        for spot in range(2 if (j, half) == (0, 0) else 0, rows * tiles // 2, 2):
            project(j, half, spot)
        if j > 0 and half == 0:
            word_copy(j).wait_recv()

    def pair_copies(i, n, which):
        return (
            send(
                part.at[i, 1],
                mate_part.at[n, which],
                pair_send.at[n, which, 0],
                pair_recv.at[n, which, 0],
                mate,
            ),
            send(
                stat.at[i, 1],
                mate_stat.at[n, which],
                pair_send.at[n, which, 1],
                pair_recv.at[n, which, 1],
                mate,
            ),
        )

    fin_copies = (
        send(both_part, fin_part, fin_send.at[0], fin_recv.at[0], partner),
        send(both_stat, fin_stat, fin_send.at[1], fin_recv.at[1], partner),
    )

    def weigh(sources):
        peaks = [ref[0:HEADS, :] for _, ref in sources]
        top = functools.reduce(jnp.maximum, peaks)
        weights = [
            jnp.exp2(peak - top) * ref[HEADS : 2 * HEADS, :]
            for peak, (_, ref) in zip(peaks, sources)
        ]
        total = functools.reduce(jnp.add, weights)
        return top, weights, total

    def mixed(sources, weights, h):
        rows_of = slice(h * head, (h + 1) * head)
        return functools.reduce(
            jnp.add,
            [
                ref[rows_of, :].astype(f32) * weight[h : h + 1, :]
                for weight, (ref, _) in zip(weights, sources)
            ],
        )

    def turn_of(j, half, which):
        if j < last:
            return j * STEPS + half * 2 + which
        return j * STEPS + FINAL.index((half, which))

    def gathered(which):
        sources = []
        for j in range(planes):
            for half in range(2):
                n = 2 * j + half
                for copy in pair_copies(0, n, which):
                    copy.wait_recv()
                i = turn_of(j, half, which)
                sources.append((part.at[i, 0], stat.at[i, 0]))
                sources.append((mate_part.at[n, which], mate_stat.at[n, which]))
        return sources

    project(0, 0, 0)
    relay()

    factor = math.log2(math.e) / math.sqrt(head)

    def queries(which, s):
        value = lax.dot_general(
            wq_t[...], qf[2 * which + s], (((1,), (1,)), ((), ())), preferred_element_type=f32
        )
        value = value.astype(jnp.bfloat16).astype(f32) * factor
        high = value.astype(jnp.bfloat16)
        low = (value - high.astype(f32)).astype(jnp.bfloat16)
        for h in range(HEADS):
            rows_of = slice(h * head, (h + 1) * head)
            q_all[which, s, h, :head, :] = high[rows_of, :]
            q_all[which, s, h, head:, :] = low[rows_of, :]

    def await_query(slot):
        send(qf.at[slot], qf.at[slot], q_send.at[0], q_recv.at[slot], mate).wait_recv()

    def turn(i, carry):
        j = i // STEPS
        u = lax.rem(i, STEPS)
        ending = j == last
        half = jnp.where(ending, pick([a for a, _ in FINAL], u), u // 2)
        which = jnp.where(ending, pick([b for _, b in FINAL], u), lax.rem(u, 2))
        n = 2 * j + half
        chip = jnp.where(which == 0, m, other)

        @pl.when(i == turn_of(0, 0, 1))
        def _():
            query_copy(1).wait_recv()
            query_copy(2).start()

        def forward(late):
            for plane in range(1, planes):
                base = (plane - 1) * STEPS
                for unit in range(tiles):
                    if SPREAD[unit] % 2 == late:

                        @pl.when(i == base + SPREAD[unit] // 2)
                        def _():
                            line_copy(plane, unit).wait_recv()
                            for copy in spread_copies(plane, unit):
                                copy.start()
                            if unit == tiles - 1:
                                word_copy(plane).start()

        forward(0)

        for plane in range(planes):
            for part_of in range(2):

                @pl.when(i == min(turn_of(plane, part_of, 0), turn_of(plane, part_of, 1)))
                def _():
                    begin(plane, part_of)

        for pair in range(2):

            @pl.when(i == turn_of(0, 0, pair))
            def _():
                queries(pair, 0)
                await_query(2 * pair + 1)
                queries(pair, 1)

        @pl.when(i == last * STEPS + 2)
        def _():
            sources = gathered(1)
            top, weights, total = weigh(sources)
            both_stat[0:HEADS, :] = top
            both_stat[HEADS : 2 * HEADS, :] = total
            for h in range(HEADS):
                both_part[h * head : (h + 1) * head, :] = (
                    mixed(sources, weights, h) / total[h : h + 1, :]
                ).astype(jnp.bfloat16)
            for copy in fin_copies:
                copy.start()

        spots = []
        for spot in range(rows * tiles // 2):
            choices = [order(0, 0)[spot], order(0, 1)[spot], order(1, 0)[spot], order(1, 1)[spot]]
            index = [row_from(d) * tiles + t for d, t in choices]
            spots.append(
                jnp.where(
                    j == 0,
                    jnp.where(half == 0, index[0], index[1]),
                    jnp.where(half == 0, index[2], index[3]),
                )
            )
        for s in range(2):
            lane = k if s == 0 else 1 - k
            first = (lax.rem(chip, 2) * 2 + lane) * tiles * k_tiles
            build_bias(words.at[j], first, k_tiles, spots, bias.at[s])

        attend(q_all.at[which], k_all.at[n], v_all.at[n], part.at[i], stat.at[i], bias, score,
            lambda: forward(1))

        for copy in pair_copies(i, n, which):
            copy.start()

        return carry

    lax.fori_loop(0, turns, turn, 0)

    numer = bias.at[0]
    sources = gathered(0)
    top, weights, total = weigh(sources)
    for h in range(HEADS):
        numer[h * head : (h + 1) * head, :] = mixed(sources, weights, h)
    for copy in fin_copies:
        copy.wait_recv()
    peak = jnp.maximum(top, fin_stat[0:HEADS, :])
    mine = jnp.exp2(top - peak)
    theirs = jnp.exp2(fin_stat[0:HEADS, :] - peak) * fin_stat[HEADS : 2 * HEADS, :]
    den = total * mine + theirs
    mine, theirs = mine / den, theirs / den
    for h in range(HEADS):
        rows_of = slice(h * head, (h + 1) * head)
        attended[rows_of, :] = (
            numer[rows_of, :] * mine[h : h + 1, :]
            + fin_part[rows_of, :].astype(f32) * theirs[h : h + 1, :]
        ).astype(jnp.bfloat16)
    out_ref[...] = lax.dot_general(
        attended[...], wo_ref[...], (((0,), (0,)), ((), ())), preferred_element_type=f32
    ).astype(jnp.bfloat16)

    for step in range(3):
        query_copy(step).wait_send()
    for j in range(planes):
        for unit in range(tiles if j else 1):
            for copy in spread_copies(j, unit) + ([] if j else relay_copies()):
                copy.wait_send()
        if j:
            for tile in range(tiles):
                line_copy(j, tile).wait_send()
            word_copy(j).wait_send()
    for n in range(2 * planes):
        for which in range(2):
            for copy in pair_copies(0, n, which):
                copy.wait_send()
    for copy in fin_copies:
        copy.wait_send()


def fused(mesh_shape, count, pairs, masks, features, w_query, w_key, w_value, w_out):
    rows, cols = mesh_shape["row"], mesh_shape["col"]
    planes = cols // 4
    turns = planes * STEPS
    nodes, width = features.shape
    keys = rows * nodes // 2
    head = width // HEADS
    tiles = nodes // TILE
    entries = 2 * 2 * tiles * rows * tiles
    bf16, f32, i32 = jnp.bfloat16, jnp.float32, jnp.int32
    whole = pl.BlockSpec(memory_space=pltpu.VMEM)
    hbm = pl.BlockSpec(memory_space=pl.ANY)
    dma = pltpu.SemaphoreType.DMA
    return pl.pallas_call(
        functools.partial(fused_kernel, rows, cols),
        out_shape=jax.ShapeDtypeStruct((nodes, w_out.shape[1]), bf16),
        in_specs=[pl.BlockSpec(memory_space=pltpu.SMEM), whole, hbm, whole] + [hbm] * 4,
        out_specs=whole,
        scratch_shapes=[
            pltpu.VMEM(masks.shape, i32),
            pltpu.VMEM((width, width), bf16),
            pltpu.VMEM((width, width), bf16),
            pltpu.VMEM((width, width), bf16),
            pltpu.VMEM(w_out.shape, bf16),
            pltpu.VMEM((planes, rows, nodes, width), bf16),
            pltpu.VMEM((4, nodes, width), bf16),
            pltpu.VMEM((width, width), bf16),
            pltpu.VMEM((width, width), bf16),
            pltpu.VMEM((TILE // 32, cols // 4 * entries, TILE), i32),
            pltpu.VMEM((planes, TILE // 32, entries, TILE), i32),
            pltpu.VMEM((2 * planes, HEADS, keys, 2 * head), bf16),
            pltpu.VMEM((2 * planes, HEADS, head + ONES, keys), bf16),
            pltpu.VMEM((2, 2, HEADS, 2 * head, nodes), bf16),
            pltpu.VMEM((turns, 2, width, nodes), bf16),
            pltpu.VMEM((turns, 2, 2 * HEADS, nodes), f32),
            pltpu.VMEM((2 * planes, 2, width, nodes), bf16),
            pltpu.VMEM((2 * planes, 2, 2 * HEADS, nodes), f32),
            pltpu.VMEM((width, nodes), bf16),
            pltpu.VMEM((2 * HEADS, nodes), f32),
            pltpu.VMEM((width, nodes), bf16),
            pltpu.VMEM((2 * HEADS, nodes), f32),
            pltpu.VMEM((width, nodes), bf16),
            pltpu.VMEM((2, keys, nodes), f32),
            pltpu.VMEM((2, 2, keys, nodes), f32),
            dma((3,)),
            dma((4,)),
            dma((planes, tiles)),
            dma((planes, tiles)),
            dma((planes, rows, rows, 2 * tiles)),
            dma((planes, rows, 2 * tiles)),
            dma((planes,)),
            dma((planes,)),
            dma((2 * planes, 2, 2)),
            dma((2 * planes, 2, 2)),
            dma((2,)),
            dma((2,)),
            dma((5,)),
        ],
        compiler_params=pltpu.CompilerParams(
            collective_id=0, has_side_effects=True, vmem_limit_bytes=67_043_328
        ),
        name="fused",
    )(count, pairs, masks, features, w_query, w_key, w_value, w_out)


def body(mesh_shape, features, w_query, w_key, w_value, w_out, pairs, counts, masks):
    words = masks[0, 0].transpose(0, 2, 1).reshape(-1, TILE)
    listed = pairs[0, 0].transpose(1, 0)
    return fused(
        mesh_shape, counts, listed, words, features, w_query, w_key, w_value, w_out
    )


def solution(mesh):
    in_specs = (
        P(("row", "col"), None),
        P(),
        P(),
        P(),
        P(),
        P("row", "col", None, None),
        P("row", "col"),
        P("row", "col", None, None, None),
    )
    out_specs = P(("row", "col"), None)
    return jax.shard_map(
        functools.partial(body, dict(mesh.shape)), mesh=mesh, in_specs=in_specs, out_specs=out_specs, check_vma=False)
```

```python
import functools
import math

import jax
import jax.numpy as jnp
from jax import lax
from jax.experimental import pallas as pl
from jax.experimental.pallas import tpu as pltpu
from jax.sharding import PartitionSpec as P

HEADS = 8
TILE = 128
BLOCK = 256
ONES = 16
MESH = pl.DeviceIdType.MESH
STEPS = 4
SPREAD = (2, 3)
FINAL = ((0, 1), (1, 1), (0, 0), (1, 0))


def build_bias(words_ref, first, k_tiles, spots, bias_ref):
    span = bias_ref.shape[1]
    tiles = span // TILE
    shift = 31 - lax.broadcasted_iota(jnp.int32, (32, TILE), 0)
    for b, spot in enumerate(spots):
        for t in range(tiles):
            cell = first + t * k_tiles + spot
            for j in range(TILE // 32):
                bits = jnp.broadcast_to(words_ref[j, pl.ds(cell, 1), :], (32, TILE)) << shift
                bias_ref[pl.ds(b * TILE + j * 32, 32), pl.ds(t * TILE, TILE)] = jnp.where(
                    bits < 0, 0.0, -jnp.inf
                )


def attend(q_ref, k_ref, v_ref, part_ref, stat_ref, bias_ref, score_ref, middle):
    heads, keys, _ = k_ref.shape
    span = q_ref.shape[3]
    head = v_ref.shape[1] - ONES
    blocks = keys // BLOCK
    zero = jnp.zeros((8, span), jnp.float32)

    def scores(h, s, block, top):
        rows = slice(block * BLOCK, (block + 1) * BLOCK)
        raw = jnp.dot(k_ref[h, rows, :], q_ref[s, h], preferred_element_type=jnp.float32)
        raw = raw + bias_ref[s, rows, :]
        score_ref[h % 2, s, rows, :] = raw
        return jnp.maximum(top, jnp.max(raw.reshape(BLOCK // 8, 8, span), axis=0))

    def weighted(h, s, block, top, total):
        rows = slice(block * BLOCK, (block + 1) * BLOCK)
        prob = jnp.exp2(score_ref[h % 2, s, rows, :] - top).astype(jnp.bfloat16)
        term = jnp.dot(v_ref[h, :, rows], prob, preferred_element_type=jnp.float32)
        return term if total is None else total + term

    def finish(h, s, top, total):
        den = total[head : head + 1, :] + jnp.exp2(-top)
        part_ref[s, h * head : (h + 1) * head, :] = (total[:head, :] / den).astype(jnp.bfloat16)
        row = h // (heads // 2) * heads + h % (heads // 2)
        stat_ref[s, row : row + 1, :] = top
        stat_ref[s, row + heads // 2 : row + heads // 2 + 1, :] = den

    tops = [zero, zero]
    for s in range(2):
        for block in range(blocks):
            tops[s] = scores(0, s, block, tops[s])
    for h in range(heads):
        if h == heads // 2:
            middle()
        later = [zero, zero]
        for s in range(2):
            top = jnp.max(tops[s], axis=0, keepdims=True)
            total = None
            for block in range(blocks):
                if h + 1 < heads:
                    later[s] = scores(h + 1, s, block, later[s])
                total = weighted(h, s, block, top, total)
            finish(h, s, top, total)
        tops = later


def pick(values, index):
    out = values[0]
    for n, value in enumerate(values[1:]):
        out = jnp.where(index == n + 1, value, out)
    return out


def fused_kernel(
    rows,
    cols,
    count_ref,
    pairs_ref,
    masks_hbm,
    features_ref,
    wq_hbm,
    wk_hbm,
    wv_hbm,
    wo_hbm,
    out_ref,
    masks_ref,
    wq_ref,
    wk_ref,
    wv_ref,
    wo_ref,
    kf,
    qf,
    wq_t,
    wv_t,
    dense,
    words,
    k_all,
    v_all,
    q_all,
    part,
    stat,
    mate_part,
    mate_stat,
    both_part,
    both_stat,
    fin_part,
    fin_stat,
    attended,
    bias,
    score,
    q_send,
    q_recv,
    z_send,
    z_recv,
    row_send,
    row_recv,
    word_send,
    word_recv,
    pair_send,
    pair_recv,
    fin_send,
    fin_recv,
    load,
):
    nodes, width = features_ref.shape
    head = width // HEADS
    f32 = jnp.float32
    chips = cols // 2
    planes = chips // 2
    last = planes - 1
    turns = planes * STEPS
    tiles = nodes // TILE
    square = rows == 4
    r, c = lax.axis_index("row"), lax.axis_index("col")
    m, k = c // 2, lax.rem(c, 2)
    other = m + 1 - 2 * lax.rem(m, 2)
    mate = (r, m * 2 + 1 - k)
    partner = (r, other * 2 + k)

    def reader(j):
        return lax.rem(m + chips - 2 * j, chips)

    def flip(place, b):
        return place + 1 - 2 * lax.rem(place, 2) if b else place

    def row_to(d):
        if rows % 2:
            return lax.rem(r + d, rows)
        return flip(lax.rem(r + d // 2 * 2, rows), d % 2)

    def row_from(d):
        if rows % 2:
            return lax.rem(r + rows - d, rows)
        return lax.rem(flip(r, d % 2) + rows - d // 2 * 2, rows)

    def send(src, dst, send_sem, recv_sem, device):
        return pltpu.make_async_remote_copy(
            src_ref=src,
            dst_ref=dst,
            send_sem=send_sem,
            recv_sem=recv_sem,
            device_id=device,
            device_id_type=MESH,
        )

    loads = [
        pltpu.make_async_copy(src, dst, load.at[n])
        for n, (src, dst) in enumerate(
            (
                (masks_hbm, masks_ref),
                (wk_hbm, wk_ref),
                (wv_hbm, wv_ref),
                (wq_hbm, wq_ref),
                (wo_hbm, wo_ref),
            )
        )
    ]
    barrier = pltpu.get_barrier_semaphore()
    peers = [mate, partner]
    peers += [(lax.rem(r + d, rows), c) for d in range(1, rows)]
    peers += [(r, reader(j) * 2 + k) for j in range(1, planes)]
    for peer in peers:
        pl.semaphore_signal(barrier, inc=1, device_id=peer, device_id_type=MESH)
    for copy in loads:
        copy.start()
    pl.semaphore_wait(barrier, len(peers))

    def query_copy(step):
        if step == 0:
            return send(features_ref, qf.at[1], q_send.at[0], q_recv.at[1], mate)
        if step == 1:
            return send(features_ref, qf.at[2], q_send.at[1], q_recv.at[2], partner)
        return send(qf.at[2], qf.at[3], q_send.at[2], q_recv.at[3], mate)

    def line_copy(j, tile):
        span = pl.ds(tile * TILE, TILE)
        return send(
            features_ref.at[span],
            kf.at[j, r, span],
            z_send.at[j, tile],
            z_recv.at[j, tile],
            (r, reader(j) * 2 + k),
        )

    def pieces(j, unit):
        if j == 0:
            return (0, TILE, 0), (TILE, TILE, 1)
        return ((unit * TILE, TILE, unit),)

    def row_copy(j, row, d, piece, own=False):
        start, size, n = piece
        span = pl.ds(start, size)
        return send(
            features_ref.at[span] if own else kf.at[j, row, span],
            kf.at[j, row, span],
            row_send.at[j, row, d, n],
            row_recv.at[j, row, n],
            (row_to(d), c),
        )

    def spread_copies(j, unit):
        own = j == 0
        if own and square:
            low, high = pieces(0, 0)
            order = [(1, high), (2, low), (1, low), (2, high)]
        else:
            order = [(d, piece) for piece in pieces(j, unit) for d in reversed(range(1, rows))]
        return [row_copy(j, r, d, piece, own) for d, piece in order]

    def relay_copies():
        if not square:
            return []
        low, high = pieces(0, 0)
        return [row_copy(0, row_from(1), 2, high), row_copy(0, row_from(2), 1, low)]

    def await_piece(j, d, piece):
        row_copy(j, row_from(d), 1, piece).wait_recv()

    def relay():
        low, high = pieces(0, 0)
        for copy, d, piece in zip(relay_copies(), (1, 2), (high, low)):
            await_piece(0, d, piece)
            copy.start()

    def late_pieces(j, half):
        if j == 0:
            low, high = pieces(0, 0)
            if square:
                return [] if half == 0 else [(1, low), (2, high), (3, low), (3, high)]
            span = range(1, rows // 2) if half == 0 else range(rows // 2, rows)
            return [(d, piece) for d in span for piece in (low, high)]
        return [(d, piece) for d in range(1, rows) for piece in pieces(j, half)]

    def order(j, half):
        if j == 0:
            if square:
                return [(0, 0), (0, 1), (1, 1), (2, 0)] if half == 0 else [(1, 0), (2, 1), (3, 0), (3, 1)]
            span = range(rows // 2) if half == 0 else range(rows // 2, rows)
            return [(d, t) for d in span for t in range(tiles)]
        return [(d, half) for d in range(rows)]

    def word_copy(j):
        return send(
            dense.at[:, own_words(j)],
            words.at[j],
            word_send.at[j],
            word_recv.at[j],
            (r, reader(j) * 2 + k),
        )

    query_copy(1).start()
    for j in range(1, planes):
        for tile in range(tiles):
            line_copy(j, tile).start()
    for copy in spread_copies(0, 0):
        copy.start()
    query_copy(0).start()

    k_tiles = rows * tiles
    entries = 2 * 2 * tiles * k_tiles

    def scatter_words():
        listed = masks_ref.shape[0] // (TILE // 32)
        cells = dense.shape[1]
        code = pairs_ref[0:1, :] * k_tiles + pairs_ref[1:2, :]
        valid = lax.broadcasted_iota(jnp.int32, (1, listed), 1) < count_ref[0, 0]
        code = jnp.broadcast_to(jnp.where(valid, code, -1), (cells, listed))
        place = jnp.where(
            code == lax.broadcasted_iota(jnp.int32, (cells, listed), 0), 1.0, 0.0
        ).astype(jnp.bfloat16)
        for w in range(TILE // 32):
            word = masks_ref[pl.ds(w, listed, stride=TILE // 32), :]
            merged = None
            for b in range(4):
                byte = ((word >> (8 * b)) & 255).astype(f32).astype(jnp.bfloat16)
                moved = jnp.dot(place, byte, preferred_element_type=f32).astype(jnp.int32) << (8 * b)
                merged = moved if merged is None else merged | moved
            dense[w] = merged

    def own_words(j):
        return pl.ds(pl.multiple_of(reader(j) // 2 * entries, entries), entries)

    for copy in loads:
        copy.wait()
    scatter_words()

    kf[0, r] = features_ref[...]
    qf[0] = features_ref[...]
    wq_t[...] = wq_ref[...].T
    wv_t[...] = wv_ref[...].T
    half_keys = rows * nodes // 2
    for n in range(2 * planes):
        v_all[n, :, head : head + ONES, :] = jnp.ones((HEADS, ONES, half_keys), jnp.bfloat16)
    words[0] = dense[:, own_words(0), :]

    def project(j, half, spot):
        block = jnp.concatenate(
            [
                kf[j, row_from(d), t * TILE : (t + 1) * TILE, :]
                for d, t in order(j, half)[spot : spot + 2]
            ],
            axis=0,
        )
        n = 2 * j + half
        lane = slice(spot * TILE, (spot + 2) * TILE)
        key = jnp.dot(block, wk_ref[...], preferred_element_type=f32)
        left = lax.broadcasted_iota(jnp.int32, (2 * TILE, 2 * head), 1) < head
        for p in range(HEADS // 2):
            both = key[:, p * 2 * head : (p + 1) * 2 * head]
            turned = pltpu.roll(both, head, 1)
            k_all[n, 2 * p, lane, :] = jnp.where(left, both, turned).astype(jnp.bfloat16)
            k_all[n, 2 * p + 1, lane, :] = jnp.where(left, turned, both).astype(jnp.bfloat16)
        value = lax.dot_general(
            wv_t[...], block, (((1,), (1,)), ((), ())), preferred_element_type=f32
        ).astype(jnp.bfloat16)
        for h in range(HEADS):
            v_all[n, h, :head, lane] = value[h * head : (h + 1) * head, :]

    def begin(j, half):
        for d, piece in late_pieces(j, half):
            await_piece(j, d, piece)
        for spot in range(2 if (j, half) == (0, 0) else 0, rows * tiles // 2, 2):
            project(j, half, spot)
        if j > 0 and half == 0:
            word_copy(j).wait_recv()

    few = HEADS // 2

    def features_of(part_of):
        return pl.ds(part_of * few * head, few * head)

    def stats_of(part_of):
        return pl.ds(part_of * HEADS, HEADS)

    def pair_copies(i, n, which, part_of):
        rows_of, stats = features_of(part_of), stats_of(part_of)
        return (
            send(
                part.at[i, 1, rows_of],
                mate_part.at[n, which, rows_of],
                pair_send.at[n, which, part_of, 0],
                pair_recv.at[n, which, part_of, 0],
                mate,
            ),
            send(
                stat.at[i, 1, stats],
                mate_stat.at[n, which, stats],
                pair_send.at[n, which, part_of, 1],
                pair_recv.at[n, which, part_of, 1],
                mate,
            ),
        )

    def fin_copies(part_of):
        rows_of, stats = features_of(part_of), stats_of(part_of)
        return (
            send(
                both_part.at[rows_of],
                fin_part.at[rows_of],
                fin_send.at[part_of, 0],
                fin_recv.at[part_of, 0],
                partner,
            ),
            send(
                both_stat.at[stats],
                fin_stat.at[stats],
                fin_send.at[part_of, 1],
                fin_recv.at[part_of, 1],
                partner,
            ),
        )

    def weigh(sources, part_of):
        low = part_of * HEADS
        peaks = [ref[low : low + few, :] for _, ref in sources]
        top = functools.reduce(jnp.maximum, peaks)
        weights = [
            jnp.exp2(peak - top) * ref[low + few : low + HEADS, :]
            for peak, (_, ref) in zip(peaks, sources)
        ]
        total = functools.reduce(jnp.add, weights)
        return top, weights, total

    def mixed(sources, weights, h):
        rows_of = slice(h * head, (h + 1) * head)
        return functools.reduce(
            jnp.add,
            [
                ref[rows_of, :].astype(f32) * weight[h % few : h % few + 1, :]
                for weight, (ref, _) in zip(weights, sources)
            ],
        )

    def turn_of(j, half, which):
        if j < last:
            return j * STEPS + half * 2 + which
        return j * STEPS + FINAL.index((half, which))

    def gathered(which, part_of):
        sources = []
        for j in range(planes):
            for half in range(2):
                n = 2 * j + half
                for copy in pair_copies(0, n, which, part_of):
                    copy.wait_recv()
                i = turn_of(j, half, which)
                sources.append((part.at[i, 0], stat.at[i, 0]))
                sources.append((mate_part.at[n, which], mate_stat.at[n, which]))
        return sources

    project(0, 0, 0)
    relay()

    factor = math.log2(math.e) / math.sqrt(head)

    def queries(which, s):
        value = lax.dot_general(
            wq_t[...], qf[2 * which + s], (((1,), (1,)), ((), ())), preferred_element_type=f32
        )
        value = value.astype(jnp.bfloat16).astype(f32) * factor
        high = value.astype(jnp.bfloat16)
        low = (value - high.astype(f32)).astype(jnp.bfloat16)
        for h in range(HEADS):
            rows_of = slice(h * head, (h + 1) * head)
            q_all[which, s, h, :head, :] = high[rows_of, :]
            q_all[which, s, h, head:, :] = low[rows_of, :]

    def await_query(slot):
        send(qf.at[slot], qf.at[slot], q_send.at[0], q_recv.at[slot], mate).wait_recv()

    def turn(i, carry):
        j = i // STEPS
        u = lax.rem(i, STEPS)
        ending = j == last
        half = jnp.where(ending, pick([a for a, _ in FINAL], u), u // 2)
        which = jnp.where(ending, pick([b for _, b in FINAL], u), lax.rem(u, 2))
        n = 2 * j + half
        chip = jnp.where(which == 0, m, other)

        @pl.when(i == turn_of(0, 0, 1))
        def _():
            query_copy(1).wait_recv()
            query_copy(2).start()

        def forward(late):
            for plane in range(1, planes):
                base = (plane - 1) * STEPS
                for unit in range(tiles):
                    if SPREAD[unit] % 2 == late:

                        @pl.when(i == base + SPREAD[unit] // 2)
                        def _():
                            line_copy(plane, unit).wait_recv()
                            for copy in spread_copies(plane, unit):
                                copy.start()
                            if unit == tiles - 1:
                                word_copy(plane).start()

        forward(0)

        def halfway():
            for copy in pair_copies(i, n, which, 0):
                copy.start()
            forward(1)

        for plane in range(planes):
            for part_of in range(2):

                @pl.when(i == min(turn_of(plane, part_of, 0), turn_of(plane, part_of, 1)))
                def _():
                    begin(plane, part_of)

        for pair in range(2):

            @pl.when(i == turn_of(0, 0, pair))
            def _():
                queries(pair, 0)
                await_query(2 * pair + 1)
                queries(pair, 1)

        @pl.when(i == last * STEPS + 2)
        def _():
            for part_of in range(2):
                sources = gathered(1, part_of)
                top, weights, total = weigh(sources, part_of)
                low = part_of * HEADS
                both_stat[low : low + few, :] = top
                both_stat[low + few : low + HEADS, :] = total
                for h in range(part_of * few, (part_of + 1) * few):
                    both_part[h * head : (h + 1) * head, :] = (
                        mixed(sources, weights, h) / total[h % few : h % few + 1, :]
                    ).astype(jnp.bfloat16)
                for copy in fin_copies(part_of):
                    copy.start()

        spots = []
        for spot in range(rows * tiles // 2):
            choices = [order(0, 0)[spot], order(0, 1)[spot], order(1, 0)[spot], order(1, 1)[spot]]
            index = [row_from(d) * tiles + t for d, t in choices]
            spots.append(
                jnp.where(
                    j == 0,
                    jnp.where(half == 0, index[0], index[1]),
                    jnp.where(half == 0, index[2], index[3]),
                )
            )
        for s in range(2):
            lane = k if s == 0 else 1 - k
            first = (lax.rem(chip, 2) * 2 + lane) * tiles * k_tiles
            build_bias(words.at[j], first, k_tiles, spots, bias.at[s])

        attend(q_all.at[which], k_all.at[n], v_all.at[n], part.at[i], stat.at[i], bias, score,
            halfway)

        for copy in pair_copies(i, n, which, 1):
            copy.start()

        return carry

    lax.fori_loop(0, turns, turn, 0)

    numer = bias.at[0]
    merged = []
    for part_of in range(2):
        sources = gathered(0, part_of)
        top, weights, total = weigh(sources, part_of)
        merged.append((top, total))
        for h in range(part_of * few, (part_of + 1) * few):
            numer[h * head : (h + 1) * head, :] = mixed(sources, weights, h)
    for part_of in range(2):
        for copy in fin_copies(part_of):
            copy.wait_recv()
        top, total = merged[part_of]
        low = part_of * HEADS
        other_top = fin_stat[low : low + few, :]
        peak = jnp.maximum(top, other_top)
        mine = jnp.exp2(top - peak)
        theirs = jnp.exp2(other_top - peak) * fin_stat[low + few : low + HEADS, :]
        den = total * mine + theirs
        mine, theirs = mine / den, theirs / den
        for h in range(part_of * few, (part_of + 1) * few):
            rows_of = slice(h * head, (h + 1) * head)
            at = h % few
            attended[rows_of, :] = (
                numer[rows_of, :] * mine[at : at + 1, :]
                + fin_part[rows_of, :].astype(f32) * theirs[at : at + 1, :]
            ).astype(jnp.bfloat16)
    out_ref[...] = lax.dot_general(
        attended[...], wo_ref[...], (((0,), (0,)), ((), ())), preferred_element_type=f32
    ).astype(jnp.bfloat16)

    for step in range(3):
        query_copy(step).wait_send()
    for j in range(planes):
        for unit in range(tiles if j else 1):
            for copy in spread_copies(j, unit) + ([] if j else relay_copies()):
                copy.wait_send()
        if j:
            for tile in range(tiles):
                line_copy(j, tile).wait_send()
            word_copy(j).wait_send()
    for part_of in range(2):
        for n in range(2 * planes):
            for which in range(2):
                for copy in pair_copies(0, n, which, part_of):
                    copy.wait_send()
        for copy in fin_copies(part_of):
            copy.wait_send()


def fused(mesh_shape, count, pairs, masks, features, w_query, w_key, w_value, w_out):
    rows, cols = mesh_shape["row"], mesh_shape["col"]
    planes = cols // 4
    turns = planes * STEPS
    nodes, width = features.shape
    keys = rows * nodes // 2
    head = width // HEADS
    tiles = nodes // TILE
    entries = 2 * 2 * tiles * rows * tiles
    bf16, f32, i32 = jnp.bfloat16, jnp.float32, jnp.int32
    whole = pl.BlockSpec(memory_space=pltpu.VMEM)
    hbm = pl.BlockSpec(memory_space=pl.ANY)
    dma = pltpu.SemaphoreType.DMA
    return pl.pallas_call(
        functools.partial(fused_kernel, rows, cols),
        out_shape=jax.ShapeDtypeStruct((nodes, w_out.shape[1]), bf16),
        in_specs=[pl.BlockSpec(memory_space=pltpu.SMEM), whole, hbm, whole] + [hbm] * 4,
        out_specs=whole,
        scratch_shapes=[
            pltpu.VMEM(masks.shape, i32),
            pltpu.VMEM((width, width), bf16),
            pltpu.VMEM((width, width), bf16),
            pltpu.VMEM((width, width), bf16),
            pltpu.VMEM(w_out.shape, bf16),
            pltpu.VMEM((planes, rows, nodes, width), bf16),
            pltpu.VMEM((4, nodes, width), bf16),
            pltpu.VMEM((width, width), bf16),
            pltpu.VMEM((width, width), bf16),
            pltpu.VMEM((TILE // 32, cols // 4 * entries, TILE), i32),
            pltpu.VMEM((planes, TILE // 32, entries, TILE), i32),
            pltpu.VMEM((2 * planes, HEADS, keys, 2 * head), bf16),
            pltpu.VMEM((2 * planes, HEADS, head + ONES, keys), bf16),
            pltpu.VMEM((2, 2, HEADS, 2 * head, nodes), bf16),
            pltpu.VMEM((turns, 2, width, nodes), bf16),
            pltpu.VMEM((turns, 2, 2 * HEADS, nodes), f32),
            pltpu.VMEM((2 * planes, 2, width, nodes), bf16),
            pltpu.VMEM((2 * planes, 2, 2 * HEADS, nodes), f32),
            pltpu.VMEM((width, nodes), bf16),
            pltpu.VMEM((2 * HEADS, nodes), f32),
            pltpu.VMEM((width, nodes), bf16),
            pltpu.VMEM((2 * HEADS, nodes), f32),
            pltpu.VMEM((width, nodes), bf16),
            pltpu.VMEM((2, keys, nodes), f32),
            pltpu.VMEM((2, 2, keys, nodes), f32),
            dma((3,)),
            dma((4,)),
            dma((planes, tiles)),
            dma((planes, tiles)),
            dma((planes, rows, rows, 2 * tiles)),
            dma((planes, rows, 2 * tiles)),
            dma((planes,)),
            dma((planes,)),
            dma((2 * planes, 2, 2, 2)),
            dma((2 * planes, 2, 2, 2)),
            dma((2, 2)),
            dma((2, 2)),
            dma((5,)),
        ],
        compiler_params=pltpu.CompilerParams(
            collective_id=0, has_side_effects=True, vmem_limit_bytes=67_043_328
        ),
        name="fused",
    )(count, pairs, masks, features, w_query, w_key, w_value, w_out)


def body(mesh_shape, features, w_query, w_key, w_value, w_out, pairs, counts, masks):
    words = masks[0, 0].transpose(0, 2, 1).reshape(-1, TILE)
    listed = pairs[0, 0].transpose(1, 0)
    return fused(
        mesh_shape, counts, listed, words, features, w_query, w_key, w_value, w_out
    )


def solution(mesh):
    in_specs = (
        P(("row", "col"), None),
        P(),
        P(),
        P(),
        P(),
        P("row", "col", None, None),
        P("row", "col"),
        P("row", "col", None, None, None),
    )
    out_specs = P(("row", "col"), None)
    return jax.shard_map(
        functools.partial(body, dict(mesh.shape)), mesh=mesh, in_specs=in_specs, out_specs=out_specs, check_vma=False)
```
